32 devices in a mesh: feat: 8 (over y, x, core), rep: 4 (over z).
Axes of the slice: x: 2, y: 2, z: 4, core: 2. Of those that a mesh axis runs over, the one named last changes fastest.
Arguments:
- features: bfloat16 [4, 8, 1024, 512], P('rep', None, 'feat'), may hold values from -6 to 6
- adjacency_one: int32 [4, 8, 5, 16, 512], P('rep'), may hold values from 0 to 65535, as said below
- pre_hidden: bfloat16 [4, 8, 256, 256], P('rep', 'feat'), may hold values from -6 to 6
- adjacency_two: int32 [4, 8, 5, 8, 256], P('rep', 'feat'), may hold values from 0 to 65535, as said below
- weight_two: bfloat16 [6, 256, 256], replicated, may hold values from -0.375 to 0.375
- out_grad: bfloat16 [4, 8, 128, 256], P('rep', 'feat'), may hold values from -6 to 6
Outputs:
- grad_w1: float32 [6, 1024, 256], P(None, 'feat')
- grad_b1: float32 [256], replicated
- grad_w2: float32 [6, 256, 256], replicated
- grad_b2: float32 [256], replicated
The draws below stay inside these ranges and needn't reach their ends.
Inputs may be any that keep to these rules, and one draw needn't show every extreme that they name: `adjacency_one`: bit k, k below 16, of word (w, n) is the entry of destination row 16 w + k and source column n; higher bits are zero; some rows are empty. `adjacency_two`: bit k, k below 16, of word (w, n) is the entry of seed row 16 w + k and source column n; higher bits are zero; some rows are empty.
All inputs are finite; a program needn't handle non-finite values.
Results may differ from the reference program's by a relative error of at most 0.0041.
Values may be sent and summed in bfloat16 or wider, within the bound.
No kernel may reach another device: no remote copies, remote signals or barrier semaphores. Data moves between devices by JAX's collectives and lax.ppermute only.
A program may use at most 128 MiB of HBM per device.

```python
import jax
import jax.numpy as jnp
from jax import lax

F = 1024
H = 256
R = 5
SEEDS = 128
DST1 = 256
NB = 512
GROUPS = 4
BATCHES = 8


def packed_bits(key, leading, row_count, col_count):
    density_key, ticket_key = jax.random.split(key)
    density = jax.random.randint(density_key, leading + (row_count, 1), 0, 5)
    ticket = jax.random.randint(ticket_key, leading + (row_count, col_count), 0, 16)
    entries = (ticket < 3 * density).astype(jnp.int32)
    grouped = entries.reshape(leading + (row_count // 16, 16, col_count))
    shifts = jnp.arange(16, dtype=jnp.int32)
    return jnp.sum(jnp.left_shift(grouped, shifts[:, None]), axis=-2).astype(jnp.int32)


def draw_adjacency_one(key, part):
    return packed_bits(jax.random.fold_in(key, 11), (GROUPS, BATCHES, R), DST1, NB)


def draw_adjacency_two(key, part):
    return packed_bits(jax.random.fold_in(key, 12), (GROUPS, BATCHES, R), SEEDS, DST1)


def shard_levels(own_key, dims, cuts, smallest, high):
    gain, own = 1.0, jax.random.fold_in(own_key, 6)
    for position, shards_of in cuts:
        heights = jnp.exp(jax.random.uniform(jax.random.fold_in(own, position), (shards_of,), jnp.float32, smallest / len(cuts), high / len(cuts)))
        gain = gain * jnp.repeat(heights, dims[position] // shards_of).reshape([-1 if axis == position else 1 for axis in range(len(dims))])
    return gain


def centred(rng, extent, scale, limit, cuts=(), held_as=jnp.bfloat16):
    drawn = scale * jax.random.normal(rng, extent, jnp.float32)
    if cuts:
        drawn = drawn * shard_levels(rng, extent, cuts, -0.22, 0.18)
    return jnp.clip(drawn, -limit, limit).astype(held_as)


def setup_inputs(seed: int = 0) -> dict:
    key_of = jax.random.split(jax.random.key(seed), 7)
    features = centred(key_of[0], (GROUPS, BATCHES, F, NB), 1.0, 6.0, ((0, 4), (2, 8)))
    adjacency_one = draw_adjacency_one(jax.random.fold_in(key_of[6], 71), 0)
    pre_hidden = centred(key_of[2], (GROUPS, BATCHES, DST1, H), 1.0, 6.0, ((0, 4), (1, 8)))
    adjacency_two = draw_adjacency_two(jax.random.fold_in(key_of[6], 71), 0)
    weight_two = centred(key_of[4], (R + 1, H, H), H ** -0.5, 0.375)
    out_grad = centred(key_of[5], (GROUPS, BATCHES, SEEDS, H), 1.0, 6.0, ((0, 4), (1, 8)))
    return dict(features=features, adjacency_one=adjacency_one, pre_hidden=pre_hidden, adjacency_two=adjacency_two, weight_two=weight_two, out_grad=out_grad)


def unpack(packed):
    shifts = jnp.arange(16, dtype=jnp.int32)
    spread = jnp.bitwise_and(jnp.right_shift(packed[..., None, :], shifts[:, None]), 1)
    dense = spread.reshape(packed.shape[:-2] + (packed.shape[-2] * 16, packed.shape[-1]))
    degree = jnp.sum(dense, axis=-1).astype(jnp.float32)
    return dense.astype(jnp.float32), 1.0 / jnp.maximum(degree, 1.0)


def reference(features, adjacency_one, pre_hidden, adjacency_two, weight_two, out_grad):
    total_batches = GROUPS * BATCHES
    factor = float(SEEDS * total_batches) ** -0.5
    feat_all = features.reshape((total_batches, F, NB))
    adj_one = adjacency_one.reshape((total_batches,) + adjacency_one.shape[2:])
    pre_all = pre_hidden.reshape((total_batches, DST1, H))
    adj_two = adjacency_two.reshape((total_batches,) + adjacency_two.shape[2:])
    grad_all = out_grad.reshape((total_batches, SEEDS, H))
    weights = weight_two.astype(jnp.float32)

    def one_batch(carry, inputs):
        panel_sum, upper_sum, bias_one, bias_two = carry
        columns, words_one, pre_rows, words_two, grad_rows = inputs
        hidden = jnp.maximum(pre_rows, 0).astype(jnp.float32)
        matrix_two, inverse_two = unpack(words_two)
        mixed = (jnp.einsum('rsd,dh->rsh', matrix_two, hidden) * inverse_two[..., None]).astype(jnp.bfloat16).astype(jnp.float32)
        scaled = grad_rows.astype(jnp.float32) * factor
        scaled_low = scaled.astype(jnp.bfloat16).astype(jnp.float32)
        grad_rel = jnp.einsum('rsh,sk->rhk', mixed, scaled_low)
        grad_self = jnp.einsum('sh,sk->hk', hidden[:SEEDS], scaled_low)
        upper_sum = upper_sum + jnp.concatenate([grad_self[None], grad_rel], 0)
        bias_two = bias_two + jnp.sum(scaled, 0)
        backed = (jnp.einsum('sk,rhk->rsh', scaled_low, weights[1:]) * inverse_two[..., None]).astype(jnp.bfloat16).astype(jnp.float32)
        spread_back = jnp.einsum('rsd,rsh->dh', matrix_two, backed)
        own_part = jnp.einsum('sk,hk->sh', scaled_low, weights[0])
        hidden_total = spread_back + jnp.pad(own_part, ((0, DST1 - SEEDS), (0, 0)))
        hidden_grad = jnp.where(pre_rows > 0, hidden_total, 0.0).astype(jnp.bfloat16).astype(jnp.float32)
        bias_one = bias_one + jnp.sum(hidden_grad, 0)
        matrix_one, inverse_one = unpack(words_one)
        column_f = columns.astype(jnp.float32)
        gathered = (jnp.einsum('rdn,fn->rdf', matrix_one, column_f) * inverse_one[..., None]).astype(jnp.bfloat16).astype(jnp.float32)
        panel_rel = jnp.einsum('rdf,dh->rfh', gathered, hidden_grad)
        panel_self = jnp.einsum('fd,dh->fh', column_f[:, :DST1], hidden_grad)
        panel_sum = panel_sum + jnp.concatenate([panel_self[None], panel_rel], 0)
        return (panel_sum, upper_sum, bias_one, bias_two), None

    start = (jnp.zeros((R + 1, F, H), jnp.float32), jnp.zeros((R + 1, H, H), jnp.float32),
             jnp.zeros((H,), jnp.float32), jnp.zeros((H,), jnp.float32))
    finals, unused = lax.scan(one_batch, start, (feat_all, adj_one, pre_all, adj_two, grad_all))
    return finals[0], finals[2], finals[1], finals[3]
```

```python
import functools

import jax
import jax.numpy as jnp
from jax import lax
from jax.experimental import pallas as pl
from jax.experimental.pallas import tpu as pltpu
from jax.sharding import PartitionSpec as P

BITS = 16
BIAS_ROWS = 16
F32 = jnp.float32
BF16 = jnp.bfloat16
NT = (((1,), (1,)), ((), ()))
TN = (((0,), (0,)), ((), ()))
VMEM = pl.BlockSpec(memory_space=pltpu.VMEM)


def dot(a, b, dims=(((1,), (0,)), ((), ()))):
    return lax.dot_general(a, b, dims, preferred_element_type=F32)


def reorder(rows):
    words = rows // BITS
    out = lax.broadcasted_iota(jnp.int32, (rows, rows), 0)
    src = lax.broadcasted_iota(jnp.int32, (rows, rows), 1)
    return jnp.where(src == BITS * (out % words) + out // words, 1.0, 0.0).astype(BF16)


def bits_two(words):
    count, cols = words.shape
    shifts = lax.broadcasted_iota(jnp.int32, (BITS, count, cols), 0)
    spread = jnp.bitwise_and(jnp.right_shift(words[None], shifts), 1)
    return spread.astype(F32).reshape(BITS * count, cols)


def split_rows(value):
    high = value.astype(BF16)
    return high.astype(F32), (value - high.astype(F32)).astype(BF16).astype(F32)


def pack_bias(one, two):
    row = lax.broadcasted_iota(jnp.int32, (BIAS_ROWS, one.shape[1]), 0)
    packed = jnp.zeros((BIAS_ROWS, one.shape[1]), F32)
    for place, part in enumerate(split_rows(one) + split_rows(two)):
        packed = jnp.where(row == place, part, packed)
    return packed.astype(BF16)


def read_bias(packed):
    rows = packed.astype(F32)
    return rows[0:1] + rows[1:2], rows[2:3] + rows[3:4]


def hidden_kernel(factor, pre_ref, words_ref, weight_ref, grad_ref, hidden_ref, bias_ref):
    relations = words_ref.shape[0]
    seeds = grad_ref.shape[0]
    pre = pre_ref[...]
    scaled = grad_ref[...].astype(F32) * factor
    low = scaled.astype(BF16)
    low_bits = dot(reorder(seeds), low).astype(BF16)
    total = None
    for r in range(relations):
        matrix = bits_two(words_ref[r])
        inverse = 1.0 / jnp.maximum(jnp.sum(matrix, axis=1, keepdims=True), 1.0)
        back = (dot(low_bits, weight_ref[r + 1], NT) * inverse).astype(BF16)
        part = dot(matrix.astype(BF16), back, TN)
        total = part if total is None else total + part
    own = dot(low, weight_ref[0], NT)
    rest = total.shape[0] - seeds
    total = total + jnp.concatenate([own, jnp.zeros((rest, own.shape[1]), F32)], 0)
    hidden_grad = jnp.where(pre.astype(F32) > 0, total, 0.0).astype(BF16)
    hidden_ref[...] = dot(reorder(total.shape[0]), hidden_grad).astype(BF16)
    bias_ref[...] = pack_bias(
        jnp.sum(hidden_grad.astype(F32), 0, keepdims=True), jnp.sum(scaled, 0, keepdims=True)
    )


def upper_kernel(factor, core_of, pre_ref, words_ref, grad_ref, bias_ref, own_ref, send_ref, sums):
    relations = words_ref.shape[0]
    seeds, width = grad_ref.shape
    low = (grad_ref[...].astype(F32) * factor).astype(BF16)
    low_bits = dot(reorder(seeds), low).astype(BF16)
    hidden = jnp.maximum(pre_ref[...].astype(F32), 0.0).astype(BF16)
    parts = sums.shape[0]
    rows = sums.shape[1]
    height = hidden.shape[1]
    per = rows // height
    for r in range(relations + 1):
        if r == 0:
            value = dot(hidden[:seeds], low, TN)
        else:
            matrix = bits_two(words_ref[r - 1])
            inverse = 1.0 / jnp.maximum(jnp.sum(matrix, axis=1, keepdims=True), 1.0)
            mixed = (dot(matrix.astype(BF16), hidden) * inverse).astype(BF16)
            value = dot(mixed, low_bits, TN)
        sums[r // per, (r % per) * height : (r % per + 1) * height] = value
    core = core_of()
    own_ref[...] = sums[core]
    other = 0 if parts == 1 else 1 - core
    send_ref[:rows] = sums[other].astype(BF16)
    send_ref[rows:] = bias_ref[...]


def pair_kernel(chip_of, own_ref, got_ref, bias_ref, *refs):
    outs, sums = refs[:-1], refs[-1]
    chips, rows, width = sums.shape
    height = own_ref.shape[0]
    total = own_ref[...] + got_ref[:height].astype(F32)
    sums[...] = total.reshape(chips, rows, width)
    one, two = read_bias(bias_ref[...])
    more_one, more_two = read_bias(got_ref[height:])
    packed = pack_bias(one + more_one, two + more_two)
    chip = chip_of()
    outs[0][:rows] = sums[chip]
    outs[0][rows:] = packed.astype(F32)
    for k in range(1, chips):
        outs[k][:rows] = sums[lax.bitwise_xor(chip, k)].astype(BF16)
        outs[k][rows:] = packed


def gather_kernel(column_ref, word_ref, power_ref, out_ref, wide, select):
    width, nodes = column_ref.shape[1:]
    relations, words = word_ref.shape[1:3]
    rows = words * BITS

    @pl.when(pl.program_id(0) == 0)
    def _():
        select[...] = reorder(rows)
        wide[width:] = jnp.ones((wide.shape[0] - width, nodes), BF16)

    column = column_ref[0]
    wide[:width] = column
    out_ref[:width] = dot(column[:, :rows], select[...], NT).astype(BF16)
    masks = lax.shift_left(
        jnp.int32(1), lax.broadcasted_iota(jnp.int32, (BITS, words, nodes), 0)
    )
    power = power_ref[0:1]
    for r in range(relations):
        spread = jnp.bitwise_and(word_ref[0, r][None], masks)
        matrix = spread.astype(F32).reshape(rows, nodes).astype(BF16)
        value = dot(wide[...], matrix, NT)
        count = value[width : width + 1] * power
        scale = power / jnp.maximum(count, 1.0)
        out_ref[(r + 1) * width : (r + 2) * width] = (value[:width] * scale).astype(BF16)


def panel_kernel(rep_of, order, gathered_ref, *refs):
    blocks, (own_ref, *outs), (stack, sums) = refs[: len(order)], refs[len(order) : -2], refs[-2:]
    height = blocks[0].shape[0]
    for block, place in zip(blocks, order):
        start = pl.multiple_of(place() * height, height)
        stack[pl.ds(start, height)] = block[...]
    total = dot(gathered_ref[...], stack[...])
    sums[...] = total.reshape(sums.shape)
    reps = sums.shape[0]
    rep = rep_of()
    own_ref[...] = sums[rep]
    for k in range(1, reps):
        outs[k - 1][...] = sums[(rep + k) % reps].astype(BF16)


def axis(name):
    return functools.partial(lax.axis_index, name)


def call(body, outs, scratch=(), flops=1000000, **keys):
    return pl.pallas_call(
        body,
        out_shape=outs,
        scratch_shapes=list(scratch),
        compiler_params=pltpu.CompilerParams(vmem_limit_bytes=56 * 1024 * 1024),
        cost_estimate=pl.CostEstimate(flops=flops, bytes_accessed=1000000, transcendentals=0),
        **keys,
    )


def shape(rows, cols, dtype):
    return jax.ShapeDtypeStruct((rows, cols), dtype)


def ring(count, step):
    return [(i, (i + step) % count) for i in range(count)]


def plane_sum_kernel(chip_of, own_ref, *refs):
    got, out, slots = refs[:-2], refs[-2], refs[-1]
    rows = out.shape[0] - BIAS_ROWS
    chip = chip_of()
    total = own_ref[:rows]
    slots[chip] = own_ref[rows:]
    for k, piece in enumerate(got, 1):
        total = total + piece[:rows].astype(F32)
        slots[lax.bitwise_xor(chip, k)] = piece[rows:].astype(F32)
    out[:rows] = total.astype(BF16)
    one, two = read_bias(slots[0])
    for j in range(1, slots.shape[0]):
        more_one, more_two = read_bias(slots[j])
        one, two = one + more_one, two + more_two
    out[rows:] = pack_bias(one, two)


def rep_sum_kernel(rep_of, own_ref, mine_ref, *refs):
    count = (len(refs) - 5) // 2
    got_panel, got_upper = refs[:count], refs[count : 2 * count]
    panel_ref, upper_ref, one_ref, two_ref, slots = refs[2 * count :]
    total = own_ref[...]
    for piece in got_panel:
        total = total + piece[...].astype(F32)
    panel_ref[...] = total.astype(BF16)
    rep = rep_of()
    slots[rep] = mine_ref[...]
    for k, piece in enumerate(got_upper, 1):
        slots[(rep + count + 1 - k) % (count + 1)] = piece[...]
    rows = upper_ref.shape[0]
    total = slots[0, :rows].astype(F32)
    one, two = read_bias(slots[0, rows:])
    for j in range(1, count + 1):
        total = total + slots[j, :rows].astype(F32)
        more_one, more_two = read_bias(slots[j, rows:])
        one, two = one + more_one, two + more_two
    upper_ref[...] = total.astype(BF16)
    one_ref[...] = one
    two_ref[...] = two


def place_kernel(order, *refs):
    blocks, out = refs[:-1], refs[-1]
    for block, place in zip(blocks, order):
        out[place()] = block[...].astype(F32)


def on_device(features, adjacency_one, pre_hidden, adjacency_two, weight_two, out_grad):
    feat = lax.axis_size("feat")
    reps = lax.axis_size("rep")
    pre, words_two, grad = pre_hidden[0, 0], adjacency_two[0, 0], out_grad[0, 0]
    columns, words_one = features[0], adjacency_one[0]
    batches, width, nodes = columns.shape
    relations, words = words_one.shape[1:3]
    rows_one = words * BITS
    hidden_rows, hidden_width = pre.shape
    seeds = grad.shape[0]
    factor = float(seeds * feat * reps) ** (-0.5)
    sets = relations + 1
    cores = 2
    chips = feat // cores
    direct = feat <= 8 and feat % cores == 0 and chips & (chips - 1) == 0

    def core_of():
        return lax.axis_index("feat") % cores

    def chip_of():
        return lax.axis_index("feat") // cores

    rep_of = axis("rep")

    hidden, bias = call(
        functools.partial(hidden_kernel, factor),
        (shape(hidden_rows, hidden_width, BF16), shape(BIAS_ROWS, hidden_width, BF16)),
    )(pre, words_two, weight_two, grad)

    power = jnp.broadcast_to(
        jnp.repeat(jnp.exp2(-jnp.arange(BITS, dtype=F32)), words)[None], (8, rows_one)
    )
    gathered = call(
        gather_kernel,
        shape(sets * width, batches * rows_one, BF16),
        (pltpu.VMEM((width + 16, nodes), BF16), pltpu.VMEM((rows_one, rows_one), BF16)),
        flops=10000000000,
        grid=(batches,),
        in_specs=[
            pl.BlockSpec((1, width, nodes), lambda b: (b, 0, 0)),
            pl.BlockSpec((1, relations, words, nodes), lambda b: (b, 0, 0, 0)),
            pl.BlockSpec((8, rows_one), lambda b: (0, 0)),
        ],
        out_specs=pl.BlockSpec((sets * width, rows_one), lambda b: (0, b)),
    )(columns, words_one, power)

    def to_chip(value, k):
        pairs = [(i, (i // cores ^ k) * cores + i % cores) for i in range(feat)]
        return lax.ppermute(value, "feat", pairs)

    def to_core(value):
        return lax.ppermute(value, "feat", [(i, i ^ 1) for i in range(feat)])

    upper_rows = sets * hidden_width
    half = upper_rows // cores
    piece = half // chips
    share = sets * width // reps

    if direct:
        blocks = [hidden] + [to_chip(hidden, k) for k in range(1, chips)]
        blocks = blocks + [to_core(block) for block in blocks]
        order = []
        for flip in range(cores):
            for k in range(chips):
                order.append(
                    lambda flip=flip, k=k: lax.bitwise_xor(
                        lax.axis_index("feat"), jnp.int32(k * cores + flip)
                    )
                )
        own_half, send_half = call(
            functools.partial(upper_kernel, factor, core_of),
            (shape(half, hidden_width, F32), shape(half + BIAS_ROWS, hidden_width, BF16)),
            (pltpu.VMEM((cores, half, hidden_width), F32),),
        )(pre, words_two, grad, bias)
        got_half = to_core(send_half)
        tall = piece + BIAS_ROWS
        pieces = call(
            functools.partial(pair_kernel, chip_of),
            (shape(tall, hidden_width, F32),) + (shape(tall, hidden_width, BF16),) * (chips - 1),
            (pltpu.VMEM((chips, piece, hidden_width), F32),),
        )(own_half, got_half, bias)
        got = [to_chip(pieces[k], k) for k in range(1, chips)]
        mine = call(
            functools.partial(plane_sum_kernel, chip_of),
            shape(tall, hidden_width, BF16),
            (pltpu.VMEM((chips, BIAS_ROWS, hidden_width), F32),),
        )(pieces[0], *got)
    else:
        blocks = [lax.all_gather(hidden, "feat", axis=0, tiled=True)]
        order = [lambda: 0]
        own_half, send_half = call(
            functools.partial(upper_kernel, factor, lambda: 0),
            (
                shape(upper_rows, hidden_width, F32),
                shape(upper_rows + BIAS_ROWS, hidden_width, BF16),
            ),
            (pltpu.VMEM((1, upper_rows, hidden_width), F32),),
        )(pre, words_two, grad, bias)
        summed, bias_sum = lax.psum((own_half, bias.astype(F32)), "feat")
        mine = jnp.concatenate([summed.astype(BF16), bias_sum.astype(BF16)], 0)
        tall = mine.shape[0]

    panels = call(
        functools.partial(panel_kernel, rep_of, order),
        (shape(share, hidden_width, F32),) + (shape(share, hidden_width, BF16),) * (reps - 1),
        (
            pltpu.VMEM((batches * rows_one, hidden_width), BF16),
            pltpu.VMEM((reps, share, hidden_width), F32),
        ),
    )(gathered, *blocks)
    got_panel = [
        lax.ppermute(panels[k], "rep", ring(reps, k)) for k in range(1, reps)
    ]
    got_upper = [lax.ppermute(mine, "rep", ring(reps, k)) for k in range(1, reps)]
    panel, upper, bias_one, bias_two = call(
        functools.partial(rep_sum_kernel, rep_of),
        (
            shape(share, hidden_width, BF16),
            shape(tall - BIAS_ROWS, hidden_width, BF16),
            shape(1, hidden_width, F32),
            shape(1, hidden_width, F32),
        ),
        (pltpu.VMEM((reps, tall, hidden_width), BF16),),
    )(panels[0], mine, *got_panel, *got_upper)

    panel_all = [panel] + [lax.ppermute(panel, "rep", ring(reps, k)) for k in range(1, reps)]
    grad_w1 = call(
        functools.partial(
            place_kernel,
            [lambda k=k: (lax.axis_index("rep") + reps - k) % reps for k in range(reps)],
        ),
        jax.ShapeDtypeStruct((reps, share, hidden_width), F32),
    )(*panel_all)
    grad_w1 = grad_w1.reshape(sets, width, hidden_width)
    if direct:
        upper_all = [upper] + [to_chip(upper, k) for k in range(1, chips)]
        upper_all = upper_all + [to_core(block) for block in upper_all]
        places = []
        for flip in range(cores):
            for k in range(chips):
                places.append(
                    lambda flip=flip, k=k: lax.bitwise_xor(core_of(), jnp.int32(flip)) * chips
                    + lax.bitwise_xor(chip_of(), jnp.int32(k))
                )
        grad_w2 = call(
            functools.partial(place_kernel, places),
            jax.ShapeDtypeStruct((feat, piece, hidden_width), F32),
        )(*upper_all)
    else:
        grad_w2 = upper.astype(F32)
    grad_w2 = grad_w2.reshape(sets, hidden_width, hidden_width)
    return (grad_w1, bias_one[0], grad_w2, bias_two[0])


def solution(mesh):
    placed = (
        P("rep", None, "feat", None),
        P("rep", None, None, None, None),
        P("rep", "feat", None, None),
        P("rep", "feat", None, None, None),
        P(),
        P("rep", "feat", None, None),
    )
    return jax.shard_map(
        on_device,
        mesh=mesh,
        in_specs=placed,
        out_specs=(P(None, "feat", None), P(), P(), P()),
        check_vma=False,
    )
```

```python
import functools

import jax
import jax.numpy as jnp
from jax import lax
from jax.experimental import pallas as pl
from jax.experimental.pallas import tpu as pltpu
from jax.sharding import PartitionSpec as P


BITS = 16
BIAS_ROWS = 16
LOADED = range(6)
F32 = jnp.float32
BF16 = jnp.bfloat16
NT = (((1,), (1,)), ((), ()))
TN = (((0,), (0,)), ((), ()))
VMEM = pl.BlockSpec(memory_space=pltpu.VMEM)


def dot(a, b, dims=(((1,), (0,)), ((), ()))):
    return lax.dot_general(a, b, dims, preferred_element_type=F32)


def reorder(rows):
    words = rows // BITS
    out = lax.broadcasted_iota(jnp.int32, (rows, rows), 0)
    src = lax.broadcasted_iota(jnp.int32, (rows, rows), 1)
    return jnp.where(src == BITS * (out % words) + out // words, 1.0, 0.0).astype(BF16)


def bits_two(words):
    count, cols = words.shape
    shifts = lax.broadcasted_iota(jnp.int32, (BITS, count, cols), 0)
    spread = jnp.bitwise_and(jnp.right_shift(words[None], shifts), 1)
    return spread.astype(F32).reshape(BITS * count, cols)


def split_rows(value):
    high = value.astype(BF16)
    return high.astype(F32), (value - high.astype(F32)).astype(BF16).astype(F32)


def pack_rows(*values):
    row = lax.broadcasted_iota(jnp.int32, (BIAS_ROWS, values[0].shape[1]), 0)
    packed = jnp.zeros(row.shape, F32)
    place = 0
    for value in values:
        for part in split_rows(value):
            packed = jnp.where(row == place, part, packed)
            place += 1
    return packed.astype(BF16)


def read_row(packed, place):
    rows = packed.astype(F32)
    return rows[2 * place : 2 * place + 1] + rows[2 * place + 1 : 2 * place + 2]


def upper_kernel(factor, core_of, *refs):
    count = len(LOADED)
    sources, own_ref, send_ref = refs[:count], refs[count], refs[count + 1]
    targets, (sums, sems) = refs[count + 2 : 2 * count + 2], refs[2 * count + 2 :]
    grad_ref, words_ref, pre_ref = targets[:3]
    copies = [
        pltpu.make_async_copy(source, target, sems.at[n])
        for n, (source, target) in enumerate(zip(sources, targets))
    ]
    for copy in copies:
        copy.start()
    for copy in copies[:3]:
        copy.wait()
    relations = words_ref.shape[0]
    seeds, width = grad_ref.shape
    scaled = grad_ref[...].astype(F32) * factor
    low = scaled.astype(BF16)
    low_bits = dot(reorder(seeds), low).astype(BF16)
    hidden = jnp.maximum(pre_ref[...].astype(F32), 0.0).astype(BF16)
    parts = sums.shape[0]
    rows = sums.shape[1]
    height = hidden.shape[1]
    per = rows // height
    for r in range(relations + 1):
        if r == 0:
            value = dot(hidden[:seeds], low, TN)
        else:
            matrix = bits_two(words_ref[r - 1])
            inverse = 1.0 / jnp.maximum(jnp.sum(matrix, axis=1, keepdims=True), 1.0)
            mixed = (dot(matrix.astype(BF16), hidden) * inverse).astype(BF16)
            value = dot(mixed, low_bits, TN)
        sums[r // per, (r % per) * height : (r % per + 1) * height] = value
    core = core_of()
    own_ref[:rows] = sums[core]
    other = 0 if parts == 1 else 1 - core
    send_ref[:rows] = sums[other]
    bias = jnp.sum(scaled, 0, keepdims=True)
    own_ref[rows:] = jnp.broadcast_to(bias, (BIAS_ROWS, width))
    send_ref[rows:] = jnp.broadcast_to(bias, (BIAS_ROWS, width))
    for copy in copies[3:]:
        copy.wait()


def hidden_kernel(factor, pre_ref, words_ref, weight_ref, grad_ref, hidden_ref):
    relations = words_ref.shape[0]
    seeds = grad_ref.shape[0]
    pre = pre_ref[...]
    low = (grad_ref[...].astype(F32) * factor).astype(BF16)
    low_bits = dot(reorder(seeds), low).astype(BF16)
    total = None
    for r in range(relations):
        matrix = bits_two(words_ref[r])
        inverse = 1.0 / jnp.maximum(jnp.sum(matrix, axis=1, keepdims=True), 1.0)
        back = (dot(low_bits, weight_ref[r + 1], NT) * inverse).astype(BF16)
        part = dot(matrix.astype(BF16), back, TN)
        total = part if total is None else total + part
    own = dot(low, weight_ref[0], NT)
    rest = total.shape[0] - seeds
    total = total + jnp.concatenate([own, jnp.zeros((rest, own.shape[1]), F32)], 0)
    hidden_grad = jnp.where(pre.astype(F32) > 0, total, 0.0).astype(BF16)
    hidden_ref[...] = dot(reorder(total.shape[0]), hidden_grad).astype(BF16)


def pair_kernel(chip_of, own_ref, got_ref, *refs):
    outs, sums = refs[:-1], refs[-1]
    chips, rows, width = sums.shape
    height = chips * rows
    total = own_ref[:height] + got_ref[:height]
    sums[...] = total.reshape(chips, rows, width)
    bias = own_ref[height:] + got_ref[height:]
    packed = pack_rows(bias[0:1])
    chip = chip_of()
    outs[0][:rows] = sums[chip]
    outs[0][rows:] = packed.astype(F32)
    for k in range(1, chips):
        outs[k][:rows] = sums[lax.bitwise_xor(chip, k)].astype(BF16)
        outs[k][rows:] = packed


def gather_kernel(first, count, column_ref, word_ref, out_ref, wide):
    width, nodes = column_ref.shape[1:]
    relations, words = word_ref.shape[1:3]
    rows = words * BITS
    select = reorder(rows)
    wide[width:] = jnp.ones((wide.shape[0] - width, nodes), BF16)
    bit = lax.broadcasted_iota(jnp.int32, (1, rows), 1) // words
    power = lax.shift_left(jnp.int32(1), BITS - 1 - bit).astype(F32) * 2.0 ** (1 - BITS)

    def batch(b):
        column = column_ref[first + b]
        wide[:width] = column
        place = pl.ds(pl.multiple_of(b * rows, rows), rows)
        out_ref[:width, place] = dot(column[:, :rows], select, NT).astype(BF16)
        for r in range(relations):
            word = word_ref[first + b, r]
            matrix = jnp.concatenate(
                [jnp.bitwise_and(word, 1 << k).astype(F32).astype(BF16) for k in range(BITS)], 0
            )
            value = dot(wide[...], matrix, NT)
            total = value[width : width + 1] * power
            scale = power / jnp.maximum(total, 1.0)
            out_ref[(r + 1) * width : (r + 2) * width, place] = (value[:width] * scale).astype(BF16)

    if count <= 4:
        for b in range(count):
            batch(b)
    else:
        lax.fori_loop(0, count, lambda b, unused: (batch(b), unused)[1], 0)


def panel_kernel(taker, order, parts, *refs):
    gathered, refs = refs[:parts], refs[parts:]
    blocks, (bias_ref, own_ref, *outs) = refs[: len(order)], refs[len(order) : -2]
    stack, sums = refs[-2:]
    height = blocks[0].shape[0]
    for block, place in zip(blocks, order):
        start = pl.multiple_of(place() * height, height)
        stack[pl.ds(start, height)] = block[...]
    deep = gathered[0].shape[1]
    total = dot(gathered[0][...], stack[:deep])
    for n in range(1, parts):
        total = total + dot(gathered[n][...], stack[n * deep : (n + 1) * deep])
    sums[...] = total.reshape(sums.shape)
    reps = sums.shape[0]
    bias_ref[...] = jnp.sum(stack[...].astype(F32), 0, keepdims=True)
    own_ref[...] = sums[taker(0)]
    for k in range(1, reps):
        outs[k - 1][...] = sums[taker(k)].astype(BF16)


def call(body, outs, scratch=(), flops=1000000, vmem=8, **keys):
    return pl.pallas_call(
        body,
        out_shape=outs,
        scratch_shapes=list(scratch),
        compiler_params=pltpu.CompilerParams(vmem_limit_bytes=vmem * 1024 * 1024),
        cost_estimate=pl.CostEstimate(flops=flops, bytes_accessed=1000000, transcendentals=0),
        **keys,
    )


def shape(rows, cols, dtype):
    return jax.ShapeDtypeStruct((rows, cols), dtype)


def plane_sum_kernel(chip_of, bias_ref, own_ref, *refs):
    got, out, slots = refs[:-2], refs[-2], refs[-1]
    rows = out.shape[0] - BIAS_ROWS
    chip = chip_of()
    total = own_ref[:rows]
    slots[chip] = own_ref[rows:]
    for k, piece in enumerate(got, 1):
        total = total + piece[:rows].astype(F32)
        slots[lax.bitwise_xor(chip, k)] = piece[rows:].astype(F32)
    out[:rows] = total
    bias = read_row(slots[0], 0)
    for j in range(1, slots.shape[0]):
        bias = bias + read_row(slots[j], 0)
    row = lax.broadcasted_iota(jnp.int32, (BIAS_ROWS, bias.shape[1]), 0)
    out[rows:] = jnp.where(row == 0, bias_ref[...], bias)


def rep_pair_kernel(mine_ref, got_ref, out_ref):
    rows = out_ref.shape[0] - BIAS_ROWS
    out_ref[:rows] = (mine_ref[:rows] + got_ref[:rows]).astype(BF16)
    bias = mine_ref[rows:] + got_ref[rows:]
    out_ref[rows:] = pack_rows(bias[0:1], bias[1:2])


def rep_more_kernel(mine_ref, got_ref, out_ref):
    rows = out_ref.shape[0] - BIAS_ROWS
    out_ref[:rows] = (mine_ref[:rows].astype(F32) + got_ref[:rows].astype(F32)).astype(BF16)
    mine, got = mine_ref[rows:], got_ref[rows:]
    out_ref[rows:] = pack_rows(
        read_row(mine, 0) + read_row(got, 0), read_row(mine, 1) + read_row(got, 1)
    )


def finish_kernel(mine_ref, got_ref, upper_ref, one_ref, two_ref):
    rows = upper_ref.shape[0]
    upper_ref[...] = (mine_ref[:rows].astype(F32) + got_ref[:rows].astype(F32)).astype(BF16)
    mine, got = mine_ref[rows:], got_ref[rows:]
    one_ref[...] = read_row(mine, 0) + read_row(got, 0)
    two_ref[...] = read_row(mine, 1) + read_row(got, 1)


def panel_sum_kernel(own_ref, *refs):
    total = own_ref[...]
    for piece in refs[:-1]:
        total = total + piece[...].astype(F32)
    refs[-1][...] = total.astype(BF16)


def layers(blocks):
    for block in blocks:
        if len(block.shape) == 2:
            yield block[...]
        else:
            for n in range(block.shape[0]):
                yield block[n]


def pack_kernel(*refs):
    for n, value in enumerate(layers(refs[:-1])):
        refs[-1][n] = value


def place_kernel(order, *refs):
    for value, place in zip(layers(refs[:-1]), order):
        refs[-1][place()] = value.astype(F32)


def on_device(features, adjacency_one, pre_hidden, adjacency_two, weight_two, out_grad):
    feat = lax.axis_size("feat")
    reps = lax.axis_size("rep")
    pre, words_two, grad = pre_hidden[0, 0], adjacency_two[0, 0], out_grad[0, 0]
    columns, words_one = features[0], adjacency_one[0]
    batches, width, nodes = columns.shape
    relations, words = words_one.shape[1:3]
    rows_one = words * BITS
    hidden_rows, hidden_width = pre.shape
    seeds = grad.shape[0]
    factor = float(seeds * feat * reps) ** (-0.5)
    sets = relations + 1
    cores = 2
    chips = feat // cores
    direct = feat <= 8 and feat % cores == 0 and chips & (chips - 1) == 0

    def core_of():
        return lax.axis_index("feat") % cores

    def chip_of():
        return lax.axis_index("feat") // cores

    def in_hbm(value):
        return pltpu.with_memory_space_constraint(value, pltpu.HBM)

    loaded = (grad, words_two, pre, weight_two, words_one, columns)
    upper_rows = sets * hidden_width
    half = upper_rows // cores if direct else upper_rows
    own_half, send_half, grad, words_two, pre, weight_two, words_one, columns = call(
        functools.partial(upper_kernel, factor, core_of if direct else lambda: 0),
        (shape(half + BIAS_ROWS, hidden_width, F32),) * 2
        + tuple(jax.ShapeDtypeStruct(v.shape, v.dtype) for v in loaded),
        [
            pltpu.VMEM((upper_rows // half, half, hidden_width), F32),
            pltpu.SemaphoreType.DMA((len(loaded),)),
        ],
        vmem=8 + sum(v.size * v.dtype.itemsize for v in loaded) // 2**20,
        in_specs=[pl.BlockSpec(memory_space=pltpu.HBM)] * len(loaded),
    )(*map(in_hbm, loaded))
    hidden = call(
        functools.partial(hidden_kernel, factor), shape(hidden_rows, hidden_width, BF16)
    )(pre, words_two, weight_two, grad)

    parts = 2 if batches % 2 == 0 else 1
    run = batches // parts
    gathered = []
    for n in range(parts):
        gathered.append(
            call(
                functools.partial(gather_kernel, n * run, run),
                shape(sets * width, run * rows_one, BF16),
                (pltpu.VMEM((width + 16, nodes), BF16),),
                flops=3000000000,
                vmem=12 + 2 * words_one.size * 4 // 2**20,
            )(columns, words_one)
        )

    def to_chip(value, k):
        pairs = [(i, (i // cores ^ k) * cores + i % cores) for i in range(feat)]
        return lax.ppermute(value, "feat", pairs)

    def to_core(value):
        return lax.ppermute(value, "feat", [(i, i ^ 1) for i in range(feat)])

    flip = reps & (reps - 1) == 0

    def giver(k):
        rep = lax.axis_index("rep")
        return lax.bitwise_xor(rep, jnp.int32(k)) if flip else (rep + reps - k) % reps

    def taker(k):
        rep = lax.axis_index("rep")
        return lax.bitwise_xor(rep, jnp.int32(k)) if flip else (rep + k) % reps

    def to_rep(value, k):
        pairs = [(i, (i ^ k) if flip else (i + k) % reps) for i in range(reps)]
        return lax.ppermute(value, "rep", pairs)

    piece = half // chips
    share = sets * width // reps

    if direct:
        blocks = [hidden] + [to_chip(hidden, k) for k in range(1, chips)]
        blocks = blocks + [to_core(block) for block in blocks]
        order = []
        for flip in range(cores):
            for k in range(chips):
                order.append(
                    lambda flip=flip, k=k: lax.bitwise_xor(
                        lax.axis_index("feat"), jnp.int32(k * cores + flip)
                    )
                )
        got_half = to_core(send_half)
        tall = piece + BIAS_ROWS
        pieces = call(
            functools.partial(pair_kernel, chip_of),
            (shape(tall, hidden_width, F32),) + (shape(tall, hidden_width, BF16),) * (chips - 1),
            (pltpu.VMEM((chips, piece, hidden_width), F32),),
        )(own_half, got_half)
        got = [to_chip(pieces[k], k) for k in range(1, chips)]
    else:
        blocks = [lax.all_gather(hidden, "feat", axis=0, tiled=True)]
        order = [lambda: 0]

    stack_bytes = batches * rows_one * (hidden_width + sets * width) * 2
    bias_one, *panels = call(
        functools.partial(panel_kernel, taker, order, parts),
        (shape(1, hidden_width, F32), shape(share, hidden_width, F32))
        + (shape(share, hidden_width, BF16),) * (reps - 1),
        (
            pltpu.VMEM((batches * rows_one, hidden_width), BF16),
            pltpu.VMEM((reps, share, hidden_width), F32),
        ),
        vmem=8 + 2 * stack_bytes // 2**20,
    )(*gathered, *blocks)
    got_panel = [to_rep(panels[k], k) for k in range(1, reps)]
    if direct:
        mine = call(
            functools.partial(plane_sum_kernel, chip_of),
            shape(piece + BIAS_ROWS, hidden_width, F32),
            (pltpu.VMEM((chips, BIAS_ROWS, hidden_width), F32),),
        )(bias_one, pieces[0], *got)
    else:
        summed = lax.psum(own_half, "feat")
        mine = jnp.concatenate([summed[:half], bias_one, summed[half + 1 :]], 0)
    tall = mine.shape[0]
    if flip and reps > 2:
        got_upper = to_rep(mine, 1)
        mine = call(rep_pair_kernel, shape(tall, hidden_width, BF16))(mine, got_upper)
        k = 2
        while k < reps // 2:
            got_upper = to_rep(mine, k)
            mine = call(rep_more_kernel, shape(tall, hidden_width, BF16))(mine, got_upper)
            k *= 2
        got_upper = to_rep(mine, k)
        upper, bias_one, bias_two = call(
            finish_kernel,
            (
                shape(tall - BIAS_ROWS, hidden_width, BF16),
                shape(1, hidden_width, F32),
                shape(1, hidden_width, F32),
            ),
        )(mine, got_upper)
    else:
        mine = lax.psum(mine, "rep")
        upper = mine[:-BIAS_ROWS].astype(BF16)
        bias_one, bias_two = mine[-BIAS_ROWS:][0:1], mine[-BIAS_ROWS:][1:2]
    panel = call(panel_sum_kernel, shape(share, hidden_width, BF16))(panels[0], *got_panel)

    if flip:
        panel_all, near = [panel], [panel]
        held = [0]
        k = reps // 2
        while k:
            if len(panel_all) > 1:
                packed = call(
                    pack_kernel,
                    jax.ShapeDtypeStruct((len(held), share, hidden_width), BF16),
                )(*near)
            else:
                packed = panel[None]
            came = to_rep(packed, k)
            near = near + [came]
            panel_all = near
            held = held + [h ^ k for h in held]
            k //= 2
    else:
        panel_all = [panel] + [to_rep(panel, k) for k in range(1, reps)]
        held = list(range(reps))
    grad_w1 = call(
        functools.partial(place_kernel, [functools.partial(giver, k) for k in held]),
        jax.ShapeDtypeStruct((reps, share, hidden_width), F32),
    )(*panel_all)
    grad_w1 = grad_w1.reshape(sets, width, hidden_width)
    if direct:
        upper_all = [upper] + [to_chip(upper, k) for k in range(1, chips)]
        upper_all = upper_all + [to_core(u) for u in upper_all]
        places = []
        for flip in range(cores):
            for k in range(chips):
                places.append(
                    lambda flip=flip, k=k: lax.bitwise_xor(core_of(), jnp.int32(flip)) * chips
                    + lax.bitwise_xor(chip_of(), jnp.int32(k))
                )
        grad_w2 = call(
            functools.partial(place_kernel, places),
            jax.ShapeDtypeStruct((feat, piece, hidden_width), F32),
        )(*upper_all)
    else:
        grad_w2 = upper.astype(F32)
    grad_w2 = grad_w2.reshape(sets, hidden_width, hidden_width)
    return (grad_w1, bias_one[0], grad_w2, bias_two[0])


def solution(mesh):
    placed = (
        P("rep", None, "feat", None),
        P("rep", None, None, None, None),
        P("rep", "feat", None, None),
        P("rep", "feat", None, None, None),
        P(),
        P("rep", "feat", None, None),
    )
    return jax.shard_map(
        on_device,
        mesh=mesh,
        in_specs=placed,
        out_specs=(P(None, "feat", None), P(), P(), P()),
        check_vma=False,
    )
```

```python
import functools

import jax
import jax.numpy as jnp
from jax import lax
from jax.experimental import pallas as pl
from jax.experimental.pallas import tpu as pltpu
from jax.sharding import PartitionSpec as P


BITS = 16
BIAS_ROWS = 16
LOADED = range(6)
F32 = jnp.float32
BF16 = jnp.bfloat16
NT = (((1,), (1,)), ((), ()))
TN = (((0,), (0,)), ((), ()))
VMEM = pl.BlockSpec(memory_space=pltpu.VMEM)


def dot(a, b, dims=(((1,), (0,)), ((), ()))):
    return lax.dot_general(a, b, dims, preferred_element_type=F32)


def reorder(rows):
    words = rows // BITS
    out = lax.broadcasted_iota(jnp.int32, (rows, rows), 0)
    src = lax.broadcasted_iota(jnp.int32, (rows, rows), 1)
    return jnp.where(src == BITS * (out % words) + out // words, 1.0, 0.0).astype(BF16)


def bits_two(words):
    count, cols = words.shape
    shifts = lax.broadcasted_iota(jnp.int32, (BITS, count, cols), 0)
    spread = jnp.bitwise_and(jnp.right_shift(words[None], shifts), 1)
    return spread.astype(F32).reshape(BITS * count, cols)


def split_rows(value):
    high = value.astype(BF16)
    return high.astype(F32), (value - high.astype(F32)).astype(BF16).astype(F32)


def pack_rows(*values):
    row = lax.broadcasted_iota(jnp.int32, (BIAS_ROWS, values[0].shape[1]), 0)
    packed = jnp.zeros(row.shape, F32)
    place = 0
    for value in values:
        for part in split_rows(value):
            packed = jnp.where(row == place, part, packed)
            place += 1
    return packed.astype(BF16)


def read_row(packed, place):
    rows = packed.astype(F32)
    return rows[2 * place : 2 * place + 1] + rows[2 * place + 1 : 2 * place + 2]


def upper_kernel(factor, core_of, *refs):
    count = len(LOADED)
    sources, own_ref, send_ref = refs[:count], refs[count], refs[count + 1]
    targets, (sums, sems) = refs[count + 2 : 2 * count + 2], refs[2 * count + 2 :]
    grad_ref, words_ref, pre_ref = targets[:3]
    copies = [
        pltpu.make_async_copy(source, target, sems.at[n])
        for n, (source, target) in enumerate(zip(sources, targets))
    ]
    for copy in copies:
        copy.start()
    for copy in copies[:3]:
        copy.wait()
    relations = words_ref.shape[0]
    seeds, width = grad_ref.shape
    scaled = grad_ref[...].astype(F32) * factor
    low = scaled.astype(BF16)
    low_bits = dot(reorder(seeds), low).astype(BF16)
    hidden = jnp.maximum(pre_ref[...].astype(F32), 0.0).astype(BF16)
    parts = sums.shape[0]
    rows = sums.shape[1]
    height = hidden.shape[1]
    per = rows // height
    for r in range(relations + 1):
        if r == 0:
            value = dot(hidden[:seeds], low, TN)
        else:
            matrix = bits_two(words_ref[r - 1])
            inverse = 1.0 / jnp.maximum(jnp.sum(matrix, axis=1, keepdims=True), 1.0)
            mixed = (dot(matrix.astype(BF16), hidden) * inverse).astype(BF16)
            value = dot(mixed, low_bits, TN)
        sums[r // per, (r % per) * height : (r % per + 1) * height] = value
    core = core_of()
    own_ref[:rows] = sums[core]
    other = 0 if parts == 1 else 1 - core
    send_ref[:rows] = sums[other]
    bias = jnp.sum(scaled, 0, keepdims=True)
    own_ref[rows:] = jnp.broadcast_to(bias, (BIAS_ROWS, width))
    send_ref[rows:] = jnp.broadcast_to(bias, (BIAS_ROWS, width))
    for copy in copies[3:]:
        copy.wait()


def hidden_kernel(factor, pre_ref, words_ref, weight_ref, grad_ref, hidden_ref):
    relations = words_ref.shape[0]
    seeds = grad_ref.shape[0]
    pre = pre_ref[...]
    low = (grad_ref[...].astype(F32) * factor).astype(BF16)
    low_bits = dot(reorder(seeds), low).astype(BF16)
    total = None
    for r in range(relations):
        matrix = bits_two(words_ref[r])
        inverse = 1.0 / jnp.maximum(jnp.sum(matrix, axis=1, keepdims=True), 1.0)
        back = (dot(low_bits, weight_ref[r + 1], NT) * inverse).astype(BF16)
        part = dot(matrix.astype(BF16), back, TN)
        total = part if total is None else total + part
    own = dot(low, weight_ref[0], NT)
    rest = total.shape[0] - seeds
    total = total + jnp.concatenate([own, jnp.zeros((rest, own.shape[1]), F32)], 0)
    hidden_grad = jnp.where(pre.astype(F32) > 0, total, 0.0).astype(BF16)
    hidden_ref[...] = dot(reorder(total.shape[0]), hidden_grad).astype(BF16)


def pair_kernel(taker, own_ref, got_ref, *refs):
    outs, sums = refs[:-1], refs[-1]
    reps, rows, width = sums.shape
    height = reps * rows
    total = own_ref[:height] + got_ref[:height]
    sums[...] = total.reshape(reps, rows, width)
    bias = own_ref[height:] + got_ref[height:]
    packed = pack_rows(bias[0:1])
    outs[0][:rows] = sums[taker(0)]
    outs[0][rows:] = packed.astype(F32)
    for k in range(1, reps):
        outs[k][:rows] = sums[taker(k)].astype(BF16)
        outs[k][rows:] = packed


def rep_sum_kernel(giver, chip_of, own_ref, *refs):
    reps, chips = refs[-1].shape[0], refs[-2].shape[0]
    got, outs, (sums, slots) = refs[: reps - 1], refs[reps - 1 : -2], refs[-2:]
    rows = sums.shape[1]
    height = chips * rows
    total = own_ref[:height]
    slots[giver(0)] = own_ref[height:]
    for k, piece in enumerate(got, 1):
        total = total + piece[:height].astype(F32)
        slots[giver(k)] = piece[height:].astype(F32)
    sums[...] = total.reshape(sums.shape)
    bias = read_row(slots[0], 0)
    for j in range(1, reps):
        bias = bias + read_row(slots[j], 0)
    packed = pack_rows(bias)
    chip = chip_of()
    outs[0][:rows] = sums[chip]
    outs[0][rows:] = packed.astype(F32)
    for k in range(1, chips):
        outs[k][:rows] = sums[lax.bitwise_xor(chip, k)].astype(BF16)
        outs[k][rows:] = packed


def gather_kernel(first, count, column_ref, word_ref, out_ref, wide):
    width, nodes = column_ref.shape[1:]
    relations, words = word_ref.shape[1:3]
    rows = words * BITS
    select = reorder(rows)
    wide[width:] = jnp.ones((wide.shape[0] - width, nodes), BF16)
    bit = lax.broadcasted_iota(jnp.int32, (1, rows), 1) // words
    power = lax.shift_left(jnp.int32(1), BITS - 1 - bit).astype(F32) * 2.0 ** (1 - BITS)

    def batch(b):
        column = column_ref[first + b]
        wide[:width] = column
        place = pl.ds(pl.multiple_of(b * rows, rows), rows)
        out_ref[:width, place] = dot(column[:, :rows], select, NT).astype(BF16)
        for r in range(relations):
            word = word_ref[first + b, r]
            matrix = jnp.concatenate(
                [jnp.bitwise_and(word, 1 << k).astype(F32).astype(BF16) for k in range(BITS)], 0
            )
            value = dot(wide[...], matrix, NT)
            total = value[width : width + 1] * power
            scale = power / jnp.maximum(total, 1.0)
            out_ref[(r + 1) * width : (r + 2) * width, place] = (value[:width] * scale).astype(BF16)

    if count <= 4:
        for b in range(count):
            batch(b)
    else:
        lax.fori_loop(0, count, lambda b, unused: (batch(b), unused)[1], 0)


def panel_kernel(taker, order, parts, *refs):
    gathered, refs = refs[:parts], refs[parts:]
    blocks, (own_ref, *outs) = refs[: len(order)], refs[len(order) : -2]
    stack, sums = refs[-2:]
    height = blocks[0].shape[0]
    for block, place in zip(blocks, order):
        start = pl.multiple_of(place() * height, height)
        stack[pl.ds(start, height)] = block[...]
    deep = gathered[0].shape[1]
    total = dot(gathered[0][...], stack[:deep])
    for n in range(1, parts):
        total = total + dot(gathered[n][...], stack[n * deep : (n + 1) * deep])
    sums[...] = total.reshape(sums.shape)
    reps = sums.shape[0]
    own_ref[...] = sums[taker(0)]
    for k in range(1, reps):
        outs[k - 1][...] = sums[taker(k)].astype(BF16)


def call(body, outs, scratch=(), flops=1000000, vmem=8, **keys):
    return pl.pallas_call(
        body,
        out_shape=outs,
        scratch_shapes=list(scratch),
        compiler_params=pltpu.CompilerParams(vmem_limit_bytes=vmem * 1024 * 1024),
        cost_estimate=pl.CostEstimate(flops=flops, bytes_accessed=1000000, transcendentals=0),
        **keys,
    )


def shape(rows, cols, dtype):
    return jax.ShapeDtypeStruct((rows, cols), dtype)


def plane_sum_kernel(chip_of, order, own_ref, *refs):
    blocks, got = refs[: len(order)], refs[len(order) : -4]
    out, two_ref, slots, rows_sum = refs[-4:]
    rows = out.shape[0] - BIAS_ROWS
    chip = chip_of()
    total = own_ref[:rows]
    slots[chip] = own_ref[rows:]
    for k, piece in enumerate(got, 1):
        total = total + piece[:rows].astype(F32)
        slots[lax.bitwise_xor(chip, k)] = piece[rows:].astype(F32)
    out[:rows] = total.astype(BF16)
    two = read_row(slots[0], 0)
    for j in range(1, slots.shape[0]):
        two = two + read_row(slots[j], 0)
    two_ref[...] = jnp.broadcast_to(two, two_ref.shape)
    for block, place in zip(blocks, order):
        rows_sum[place()] = jnp.sum(block[...].astype(F32), 0, keepdims=True)
    one = rows_sum[0]
    for j in range(1, len(order)):
        one = one + rows_sum[j]
    out[rows:] = pack_rows(one)


def rep_join_kernel(giver, *refs):
    parts, (out, one_ref, slots) = refs[:-3], refs[-3:]
    rows = out.shape[1]
    for k, part in enumerate(parts):
        out[giver(k)] = part[:rows]
        slots[giver(k)] = part[rows:]
    one = read_row(slots[0], 0)
    for j in range(1, len(parts)):
        one = one + read_row(slots[j], 0)
    one_ref[...] = jnp.broadcast_to(one, one_ref.shape)


def panel_sum_kernel(own_ref, *refs):
    total = own_ref[...]
    for piece in refs[:-1]:
        total = total + piece[...].astype(F32)
    refs[-1][...] = total.astype(BF16)


def place_kernel(order, *refs):
    blocks, (out, held, sems) = refs[:-3], refs[-3:]
    copies = []
    for n, (block, place) in enumerate(zip(blocks, order)):
        held[n] = block[...].astype(F32)
        copies.append(pltpu.make_async_copy(held.at[n], out.at[place()], sems.at[n]))
        copies[-1].start()
    for copy in copies:
        copy.wait()


def place_two_kernel(order, *refs):
    blocks, (one_ref, two_ref) = refs[: len(order)], refs[len(order) : len(order) + 2]
    out, one_out, two_out, held, sems = refs[len(order) + 2 :]
    copies = [
        pltpu.make_async_copy(one_ref.at[0], one_out, sems.at[len(order)]),
        pltpu.make_async_copy(two_ref.at[0], two_out, sems.at[len(order) + 1]),
    ]
    for copy in copies:
        copy.start()
    for n, (block, place) in enumerate(zip(blocks, order)):
        core, chip = place()
        held[n] = block[...].astype(F32)
        copies.append(pltpu.make_async_copy(held.at[n], out.at[core, :, chip], sems.at[n]))
        copies[-1].start()
    for copy in copies:
        copy.wait()


def on_device(features, adjacency_one, pre_hidden, adjacency_two, weight_two, out_grad):
    feat = lax.axis_size("feat")
    reps = lax.axis_size("rep")
    pre, words_two, grad = pre_hidden[0, 0], adjacency_two[0, 0], out_grad[0, 0]
    columns, words_one = features[0], adjacency_one[0]
    batches, width, nodes = columns.shape
    relations, words = words_one.shape[1:3]
    rows_one = words * BITS
    hidden_rows, hidden_width = pre.shape
    seeds = grad.shape[0]
    factor = float(seeds * feat * reps) ** (-0.5)
    sets = relations + 1
    cores = 2
    chips = feat // cores
    direct = feat <= 8 and feat % cores == 0 and chips & (chips - 1) == 0
    direct = direct and sets * hidden_width % (8 * feat * reps) == 0

    def core_of():
        return lax.axis_index("feat") % cores

    def chip_of():
        return lax.axis_index("feat") // cores

    def in_hbm(value):
        return pltpu.with_memory_space_constraint(value, pltpu.HBM)

    loaded = (grad, words_two, pre, weight_two, words_one, columns)
    upper_rows = sets * hidden_width
    half = upper_rows // cores if direct else upper_rows
    own_half, send_half, grad, words_two, pre, weight_two, words_one, columns = call(
        functools.partial(upper_kernel, factor, core_of if direct else lambda: 0),
        (shape(half + BIAS_ROWS, hidden_width, F32),) * 2
        + tuple(jax.ShapeDtypeStruct(v.shape, v.dtype) for v in loaded),
        [
            pltpu.VMEM((upper_rows // half, half, hidden_width), F32),
            pltpu.SemaphoreType.DMA((len(loaded),)),
        ],
        vmem=8 + sum(v.size * v.dtype.itemsize for v in loaded) // 2**20,
        in_specs=[pl.BlockSpec(memory_space=pltpu.HBM)] * len(loaded),
    )(*map(in_hbm, loaded))
    hidden = call(
        functools.partial(hidden_kernel, factor), shape(hidden_rows, hidden_width, BF16)
    )(pre, words_two, weight_two, grad)

    parts = 2 if batches % 2 == 0 else 1
    run = batches // parts
    gathered = []
    for n in range(parts):
        gathered.append(
            call(
                functools.partial(gather_kernel, n * run, run),
                shape(sets * width, run * rows_one, BF16),
                (pltpu.VMEM((width + 16, nodes), BF16),),
                flops=3000000000,
                vmem=12 + 2 * words_one.size * 4 // 2**20,
            )(columns, words_one)
        )

    def to_chip(value, k):
        pairs = [(i, (i // cores ^ k) * cores + i % cores) for i in range(feat)]
        return lax.ppermute(value, "feat", pairs)

    def to_core(value):
        return lax.ppermute(value, "feat", [(i, i ^ 1) for i in range(feat)])

    flip = reps & (reps - 1) == 0

    def giver(k):
        rep = lax.axis_index("rep")
        return lax.bitwise_xor(rep, jnp.int32(k)) if flip else (rep + reps - k) % reps

    def taker(k):
        rep = lax.axis_index("rep")
        return lax.bitwise_xor(rep, jnp.int32(k)) if flip else (rep + k) % reps

    def to_rep(value, k):
        pairs = [(i, (i ^ k) if flip else (i + k) % reps) for i in range(reps)]
        return lax.ppermute(value, "rep", pairs)

    piece = half // (chips * reps)
    share = sets * width // reps

    if direct:
        blocks = [hidden] + [to_chip(hidden, k) for k in range(1, chips)]
        blocks = blocks + [to_core(block) for block in blocks]
        order = []
        for flip in range(cores):
            for k in range(chips):
                order.append(
                    lambda flip=flip, k=k: lax.bitwise_xor(
                        lax.axis_index("feat"), jnp.int32(k * cores + flip)
                    )
                )
        got_half = to_core(send_half)
        tall = half // reps + BIAS_ROWS
        thirds = call(
            functools.partial(pair_kernel, taker),
            (shape(tall, hidden_width, F32),) + (shape(tall, hidden_width, BF16),) * (reps - 1),
            (pltpu.VMEM((reps, half // reps, hidden_width), F32),),
        )(own_half, got_half)
        got = [to_rep(thirds[k], k) for k in range(1, reps)]
        tall = piece + BIAS_ROWS
        pieces = call(
            functools.partial(rep_sum_kernel, giver, chip_of),
            (shape(tall, hidden_width, F32),) + (shape(tall, hidden_width, BF16),) * (chips - 1),
            (
                pltpu.VMEM((chips, piece, hidden_width), F32),
                pltpu.VMEM((reps, BIAS_ROWS, hidden_width), F32),
            ),
        )(thirds[0], *got)
        got = [to_chip(pieces[k], k) for k in range(1, chips)]
    else:
        blocks = [lax.all_gather(hidden, "feat", axis=0, tiled=True)]
        order = [lambda: 0]

    stack_bytes = batches * rows_one * (hidden_width + sets * width) * 2
    panels = call(
        functools.partial(panel_kernel, taker, order, parts),
        (shape(share, hidden_width, F32),) + (shape(share, hidden_width, BF16),) * (reps - 1),
        (
            pltpu.VMEM((batches * rows_one, hidden_width), BF16),
            pltpu.VMEM((reps, share, hidden_width), F32),
        ),
        vmem=8 + 2 * stack_bytes // 2**20,
    )(*gathered, *blocks)
    got_panel = [to_rep(panels[k], k) for k in range(1, reps)]
    if direct:
        mine, bias_two = call(
            functools.partial(plane_sum_kernel, chip_of, order),
            (shape(tall, hidden_width, BF16), shape(8, hidden_width, F32)),
            (
                pltpu.VMEM((chips, BIAS_ROWS, hidden_width), F32),
                pltpu.VMEM((feat, 1, hidden_width), F32),
            ),
        )(pieces[0], *blocks, *got)
        got = [to_rep(mine, k) for k in range(1, reps)]
        upper, bias_one = call(
            functools.partial(rep_join_kernel, giver),
            (jax.ShapeDtypeStruct((reps, piece, hidden_width), BF16), shape(8, hidden_width, F32)),
            (pltpu.VMEM((reps, BIAS_ROWS, hidden_width), BF16),),
        )(mine, *got)
    else:
        summed = lax.psum(own_half, ("feat", "rep"))
        upper, bias_two = summed[:half], summed[half : half + 1]
        bias_one = lax.psum(jnp.sum(blocks[0].astype(F32), 0, keepdims=True), "rep")
    panel = call(panel_sum_kernel, shape(share, hidden_width, BF16))(panels[0], *got_panel)

    panel_all = [panel] + [to_rep(panel, k) for k in range(1, reps)]
    grad_w1 = call(
        functools.partial(place_kernel, [functools.partial(giver, k) for k in range(reps)]),
        jax.ShapeDtypeStruct((reps, share, hidden_width), F32),
        (
            pltpu.VMEM((reps, share, hidden_width), F32),
            pltpu.SemaphoreType.DMA((reps,)),
        ),
        out_specs=pl.BlockSpec(memory_space=pltpu.HBM),
    )(*panel_all)
    grad_w1 = grad_w1.reshape(sets, width, hidden_width)
    if direct:
        upper_all = [upper] + [to_chip(upper, k) for k in range(1, chips)]
        upper_all = upper_all + [to_core(u) for u in upper_all]
        places = []
        for turn in range(cores):
            for k in range(chips):
                places.append(
                    lambda turn=turn, k=k: (
                        lax.bitwise_xor(core_of(), jnp.int32(turn)),
                        lax.bitwise_xor(chip_of(), jnp.int32(k)),
                    )
                )
        grad_w2, bias_one, bias_two = call(
            functools.partial(place_two_kernel, places),
            (
                jax.ShapeDtypeStruct((cores, reps, chips, piece, hidden_width), F32),
                jax.ShapeDtypeStruct((hidden_width,), F32),
                jax.ShapeDtypeStruct((hidden_width,), F32),
            ),
            (
                pltpu.VMEM((feat, reps, piece, hidden_width), F32),
                pltpu.SemaphoreType.DMA((feat + 2,)),
            ),
            out_specs=[pl.BlockSpec(memory_space=pltpu.HBM)] * 3,
        )(*upper_all, bias_one, bias_two)
    else:
        grad_w2, bias_one, bias_two = upper, bias_one[0], bias_two[0]
    grad_w2 = grad_w2.reshape(sets, hidden_width, hidden_width)
    return (grad_w1, bias_one, grad_w2, bias_two)


def solution(mesh):
    placed = (
        P("rep", None, "feat", None),
        P("rep", None, None, None, None),
        P("rep", "feat", None, None),
        P("rep", "feat", None, None, None),
        P(),
        P("rep", "feat", None, None),
    )
    return jax.shard_map(
        on_device,
        mesh=mesh,
        in_specs=placed,
        out_specs=(P(None, "feat", None), P(), P(), P()),
        check_vma=False,
    )
```

```python
import functools

import jax
import jax.numpy as jnp
from jax import lax
from jax.experimental import pallas as pl
from jax.experimental.pallas import tpu as pltpu
from jax.sharding import PartitionSpec as P


BITS = 16
BIAS_ROWS = 16
LOADED = range(6)
FIRST_SHARE = 5
F32 = jnp.float32
BF16 = jnp.bfloat16
NT = (((1,), (1,)), ((), ()))
TN = (((0,), (0,)), ((), ()))
VMEM = pl.BlockSpec(memory_space=pltpu.VMEM)


def dot(a, b, dims=(((1,), (0,)), ((), ()))):
    return lax.dot_general(a, b, dims, preferred_element_type=F32)


def reorder(rows):
    words = rows // BITS
    out = lax.broadcasted_iota(jnp.int32, (rows, rows), 0)
    src = lax.broadcasted_iota(jnp.int32, (rows, rows), 1)
    return jnp.where(src == BITS * (out % words) + out // words, 1.0, 0.0).astype(BF16)


def bits_two(words):
    count, cols = words.shape
    shifts = lax.broadcasted_iota(jnp.int32, (BITS, count, cols), 0)
    spread = jnp.bitwise_and(jnp.right_shift(words[None], shifts), 1)
    return spread.astype(F32).reshape(BITS * count, cols)


def split_rows(value):
    high = value.astype(BF16)
    return high.astype(F32), (value - high.astype(F32)).astype(BF16).astype(F32)


def pack_rows(*values):
    row = lax.broadcasted_iota(jnp.int32, (BIAS_ROWS, values[0].shape[1]), 0)
    packed = jnp.zeros(row.shape, F32)
    place = 0
    for value in values:
        for part in split_rows(value):
            packed = jnp.where(row == place, part, packed)
            place += 1
    return packed.astype(BF16)


def read_row(packed, place):
    rows = packed.astype(F32)
    return rows[2 * place : 2 * place + 1] + rows[2 * place + 1 : 2 * place + 2]


def upper_kernel(factor, core_of, *refs):
    count = len(LOADED)
    sources, (hidden_ref, own_ref, send_ref) = refs[:count], refs[count : count + 3]
    targets, (sums, sems) = refs[count + 5 : -2] + refs[count + 3 : count + 5], refs[-2:]
    weight_ref = targets[3]
    grad_ref, words_ref, pre_ref = targets[:3]
    copies = [
        pltpu.make_async_copy(source, target, sems.at[n])
        for n, (source, target) in enumerate(zip(sources, targets))
    ]
    for copy in copies:
        copy.start()
    for copy in copies[:4]:
        copy.wait()
    relations = words_ref.shape[0]
    seeds, width = grad_ref.shape
    scaled = grad_ref[...].astype(F32) * factor
    low = scaled.astype(BF16)
    low_bits = dot(reorder(seeds), low).astype(BF16)
    pre = pre_ref[...].astype(F32)
    hidden = jnp.maximum(pre, 0.0).astype(BF16)
    parts = sums.shape[0]
    rows = sums.shape[1]
    height = hidden.shape[1]
    per = rows // height
    own = dot(low, weight_ref[0], NT)
    total = jnp.concatenate([own, jnp.zeros((pre.shape[0] - seeds, own.shape[1]), F32)], 0)
    sums[0, :height] = dot(hidden[:seeds], low, TN)
    for r in range(1, relations + 1):
        spread = bits_two(words_ref[r - 1])
        inverse = 1.0 / jnp.maximum(jnp.sum(spread, axis=1, keepdims=True), 1.0)
        matrix = spread.astype(BF16)
        back = (dot(low_bits, weight_ref[r], NT) * inverse).astype(BF16)
        total = total + dot(matrix, back, TN)
        mixed = (dot(matrix, hidden) * inverse).astype(BF16)
        sums[r // per, (r % per) * height : (r % per + 1) * height] = dot(mixed, low_bits, TN)
    hidden_grad = jnp.where(pre > 0, total, 0.0).astype(BF16)
    hidden_ref[...] = dot(reorder(total.shape[0]), hidden_grad).astype(BF16)
    core = core_of()
    own_ref[:rows] = sums[core]
    other = 0 if parts == 1 else 1 - core
    send_ref[:rows] = sums[other]
    bias = jnp.sum(scaled, 0, keepdims=True)
    own_ref[rows:] = jnp.broadcast_to(bias, (BIAS_ROWS, width))
    send_ref[rows:] = jnp.broadcast_to(bias, (BIAS_ROWS, width))
    for copy in copies[4:]:
        copy.wait()


def pair_kernel(taker, own_ref, got_ref, *refs):
    outs, sums = refs[:-1], refs[-1]
    reps, rows, width = sums.shape
    height = reps * rows
    total = own_ref[:height] + got_ref[:height]
    sums[...] = total.reshape(reps, rows, width)
    bias = own_ref[height:] + got_ref[height:]
    packed = pack_rows(bias[0:1])
    outs[0][:rows] = sums[taker(0)]
    outs[0][rows:] = packed.astype(F32)
    for k in range(1, reps):
        outs[k][:rows] = sums[taker(k)].astype(BF16)
        outs[k][rows:] = packed


def rep_sum_kernel(giver, chip_of, own_ref, *refs):
    reps, chips = refs[-1].shape[0], refs[-2].shape[0]
    got, outs, (sums, slots) = refs[: reps - 1], refs[reps - 1 : -2], refs[-2:]
    rows = sums.shape[1]
    height = chips * rows
    total = own_ref[:height]
    slots[giver(0)] = own_ref[height:]
    for k, piece in enumerate(got, 1):
        total = total + piece[:height].astype(F32)
        slots[giver(k)] = piece[height:].astype(F32)
    sums[...] = total.reshape(sums.shape)
    bias = read_row(slots[0], 0)
    for j in range(1, reps):
        bias = bias + read_row(slots[j], 0)
    packed = pack_rows(bias)
    chip = chip_of()
    outs[0][:rows] = sums[chip]
    outs[0][rows:] = packed.astype(F32)
    for k in range(1, chips):
        outs[k][:rows] = sums[lax.bitwise_xor(chip, k)].astype(BF16)
        outs[k][rows:] = packed


def gather_kernel(first, count, column_ref, word_ref, out_ref, wide):
    width, nodes = column_ref.shape[1:]
    relations, words = word_ref.shape[1:3]
    rows = words * BITS
    select = reorder(rows)
    wide[width:] = jnp.ones((wide.shape[0] - width, nodes), BF16)
    bit = lax.broadcasted_iota(jnp.int32, (1, rows), 1) // words
    power = lax.shift_left(jnp.int32(1), BITS - 1 - bit).astype(F32) * 2.0 ** (1 - BITS)

    def batch(b):
        column = column_ref[first + b]
        wide[:width] = column
        place = pl.ds(pl.multiple_of(b * rows, rows), rows)
        out_ref[:width, place] = dot(column[:, :rows], select, NT).astype(BF16)
        for r in range(relations):
            word = word_ref[first + b, r]
            matrix = jnp.concatenate(
                [jnp.bitwise_and(word, 1 << k).astype(F32).astype(BF16) for k in range(BITS)], 0
            )
            value = dot(wide[...], matrix, NT)
            total = value[width : width + 1] * power
            scale = power / jnp.maximum(total, 1.0)
            out_ref[(r + 1) * width : (r + 2) * width, place] = (value[:width] * scale).astype(BF16)

    if count <= 8:
        for b in range(count):
            batch(b)
    else:
        lax.fori_loop(0, count, lambda b, unused: (batch(b), unused)[1], 0)


def panel_kernel(taker, order, parts, *refs):
    gathered, refs = refs[:parts], refs[parts:]
    blocks, (own_ref, *outs) = refs[: len(order)], refs[len(order) : -2]
    stack, sums = refs[-2:]
    height = blocks[0].shape[0]
    for block, place in zip(blocks, order):
        start = pl.multiple_of(place() * height, height)
        stack[pl.ds(start, height)] = block[...]
    total, place = None, 0
    for part in gathered:
        deep = part.shape[1]
        value = dot(part[...], stack[place : place + deep])
        total = value if total is None else total + value
        place += deep
    sums[...] = total.reshape(sums.shape)
    reps = sums.shape[0]
    own_ref[...] = sums[taker(0)]
    for k in range(1, reps):
        outs[k - 1][...] = sums[taker(k)].astype(BF16)


def call(body, outs, scratch=(), flops=1000000, vmem=8, **keys):
    return pl.pallas_call(
        body,
        out_shape=outs,
        scratch_shapes=list(scratch),
        compiler_params=pltpu.CompilerParams(vmem_limit_bytes=vmem * 1024 * 1024),
        cost_estimate=pl.CostEstimate(flops=flops, bytes_accessed=1000000, transcendentals=0),
        **keys,
    )


def shape(rows, cols, dtype):
    return jax.ShapeDtypeStruct((rows, cols), dtype)


def plane_sum_kernel(chip_of, order, own_ref, *refs):
    blocks, got = refs[: len(order)], refs[len(order) : -4]
    out, two_ref, slots, rows_sum = refs[-4:]
    rows = out.shape[0] - BIAS_ROWS
    chip = chip_of()
    total = own_ref[:rows]
    slots[chip] = own_ref[rows:]
    for k, piece in enumerate(got, 1):
        total = total + piece[:rows].astype(F32)
        slots[lax.bitwise_xor(chip, k)] = piece[rows:].astype(F32)
    out[:rows] = total.astype(BF16)
    two = read_row(slots[0], 0)
    for j in range(1, slots.shape[0]):
        two = two + read_row(slots[j], 0)
    two_ref[...] = jnp.broadcast_to(two, two_ref.shape)
    for block, place in zip(blocks, order):
        rows_sum[place()] = jnp.sum(block[...].astype(F32), 0, keepdims=True)
    one = rows_sum[0]
    for j in range(1, len(order)):
        one = one + rows_sum[j]
    out[rows:] = pack_rows(one)


def rep_join_kernel(giver, *refs):
    parts, (out, one_ref, slots) = refs[:-3], refs[-3:]
    rows = out.shape[1]
    for k, part in enumerate(parts):
        out[giver(k)] = part[:rows]
        slots[giver(k)] = part[rows:]
    one = read_row(slots[0], 0)
    for j in range(1, len(parts)):
        one = one + read_row(slots[j], 0)
    one_ref[...] = jnp.broadcast_to(one, one_ref.shape)


def panel_sum_kernel(own_ref, *refs):
    total = own_ref[...]
    for piece in refs[:-1]:
        total = total + piece[...].astype(F32)
    refs[-1][...] = total.astype(BF16)


def place_kernel(order, *refs):
    blocks, (out, held, sems) = refs[:-3], refs[-3:]
    copies = []
    for n, (block, place) in enumerate(zip(blocks, order)):
        held[n] = block[...].astype(F32)
        copies.append(pltpu.make_async_copy(held.at[n], out.at[place()], sems.at[n]))
        copies[-1].start()
    for copy in copies:
        copy.wait()


def place_two_kernel(order, *refs):
    blocks, (one_ref, two_ref) = refs[: len(order)], refs[len(order) : len(order) + 2]
    out, one_out, two_out, held, sems = refs[len(order) + 2 :]
    copies = [
        pltpu.make_async_copy(one_ref.at[0], one_out, sems.at[len(order)]),
        pltpu.make_async_copy(two_ref.at[0], two_out, sems.at[len(order) + 1]),
    ]
    for copy in copies:
        copy.start()
    for n, (block, place) in enumerate(zip(blocks, order)):
        core, chip = place()
        held[n] = block[...].astype(F32)
        copies.append(pltpu.make_async_copy(held.at[n], out.at[core, :, chip], sems.at[n]))
        copies[-1].start()
    for copy in copies:
        copy.wait()


def on_device(features, adjacency_one, pre_hidden, adjacency_two, weight_two, out_grad):
    feat = lax.axis_size("feat")
    reps = lax.axis_size("rep")
    pre, words_two, grad = pre_hidden[0, 0], adjacency_two[0, 0], out_grad[0, 0]
    columns, words_one = features[0], adjacency_one[0]
    batches, width, nodes = columns.shape
    relations, words = words_one.shape[1:3]
    rows_one = words * BITS
    hidden_rows, hidden_width = pre.shape
    seeds = grad.shape[0]
    factor = float(seeds * feat * reps) ** (-0.5)
    sets = relations + 1
    cores = 2
    chips = feat // cores
    direct = feat <= 8 and feat % cores == 0 and chips & (chips - 1) == 0
    direct = direct and sets * hidden_width % (8 * feat * reps) == 0

    def core_of():
        return lax.axis_index("feat") % cores

    def chip_of():
        return lax.axis_index("feat") // cores

    def in_hbm(value):
        return pltpu.with_memory_space_constraint(value, pltpu.HBM)

    loaded = (grad, words_two, pre, weight_two, words_one, columns)
    upper_rows = sets * hidden_width
    half = upper_rows // cores if direct else upper_rows
    kept = (words_one, columns)
    hidden, own_half, send_half, words_one, columns = call(
        functools.partial(upper_kernel, factor, core_of if direct else lambda: 0),
        (shape(hidden_rows, hidden_width, BF16),)
        + (shape(half + BIAS_ROWS, hidden_width, F32),) * 2
        + tuple(jax.ShapeDtypeStruct(v.shape, v.dtype) for v in kept),
        [pltpu.VMEM(v.shape, v.dtype) for v in loaded[:4]]
        + [
            pltpu.VMEM((upper_rows // half, half, hidden_width), F32),
            pltpu.SemaphoreType.DMA((len(loaded),)),
        ],
        vmem=8 + sum(v.size * v.dtype.itemsize for v in loaded) // 2**20,
        in_specs=[pl.BlockSpec(memory_space=pltpu.HBM)] * len(loaded),
    )(*map(in_hbm, loaded))

    first = batches * FIRST_SHARE // 8
    runs = [(0, first), (first, batches - first)]
    gathered = []
    for start, run in runs:
        gathered.append(
            call(
                functools.partial(gather_kernel, start, run),
                shape(sets * width, run * rows_one, BF16),
                (pltpu.VMEM((width + 16, nodes), BF16),),
                flops=3000000000,
                vmem=12 + 2 * words_one.size * 4 // 2**20,
            )(columns, words_one)
        )

    def to_chip(value, k):
        pairs = [(i, (i // cores ^ k) * cores + i % cores) for i in range(feat)]
        return lax.ppermute(value, "feat", pairs)

    def to_core(value):
        return lax.ppermute(value, "feat", [(i, i ^ 1) for i in range(feat)])

    flip = reps & (reps - 1) == 0

    def giver(k):
        rep = lax.axis_index("rep")
        return lax.bitwise_xor(rep, jnp.int32(k)) if flip else (rep + reps - k) % reps

    def taker(k):
        rep = lax.axis_index("rep")
        return lax.bitwise_xor(rep, jnp.int32(k)) if flip else (rep + k) % reps

    def to_rep(value, k):
        pairs = [(i, (i ^ k) if flip else (i + k) % reps) for i in range(reps)]
        return lax.ppermute(value, "rep", pairs)

    piece = half // (chips * reps)
    share = sets * width // reps

    if direct:
        blocks = [hidden] + [to_chip(hidden, k) for k in range(1, chips)]
        blocks = blocks + [to_core(block) for block in blocks]
        order = []
        for flip in range(cores):
            for k in range(chips):
                order.append(
                    lambda flip=flip, k=k: lax.bitwise_xor(
                        lax.axis_index("feat"), jnp.int32(k * cores + flip)
                    )
                )
        got_half = to_core(send_half)
        tall = half // reps + BIAS_ROWS
        thirds = call(
            functools.partial(pair_kernel, taker),
            (shape(tall, hidden_width, F32),) + (shape(tall, hidden_width, BF16),) * (reps - 1),
            (pltpu.VMEM((reps, half // reps, hidden_width), F32),),
        )(own_half, got_half)
        got = [to_rep(thirds[k], k) for k in range(1, reps)]
        tall = piece + BIAS_ROWS
        pieces = call(
            functools.partial(rep_sum_kernel, giver, chip_of),
            (shape(tall, hidden_width, F32),) + (shape(tall, hidden_width, BF16),) * (chips - 1),
            (
                pltpu.VMEM((chips, piece, hidden_width), F32),
                pltpu.VMEM((reps, BIAS_ROWS, hidden_width), F32),
            ),
        )(thirds[0], *got)
        got = [to_chip(pieces[k], k) for k in range(1, chips)]
    else:
        blocks = [lax.all_gather(hidden, "feat", axis=0, tiled=True)]
        order = [lambda: 0]

    stack_bytes = batches * rows_one * (hidden_width + sets * width) * 2
    panels = call(
        functools.partial(panel_kernel, taker, order, len(runs)),
        (shape(share, hidden_width, F32),) + (shape(share, hidden_width, BF16),) * (reps - 1),
        (
            pltpu.VMEM((batches * rows_one, hidden_width), BF16),
            pltpu.VMEM((reps, share, hidden_width), F32),
        ),
        vmem=8 + 2 * stack_bytes // 2**20,
    )(*gathered, *blocks)
    got_panel = [to_rep(panels[k], k) for k in range(1, reps)]
    if direct:
        mine, bias_two = call(
            functools.partial(plane_sum_kernel, chip_of, order),
            (shape(tall, hidden_width, BF16), shape(8, hidden_width, F32)),
            (
                pltpu.VMEM((chips, BIAS_ROWS, hidden_width), F32),
                pltpu.VMEM((feat, 1, hidden_width), F32),
            ),
        )(pieces[0], *blocks, *got)
        got = [to_rep(mine, k) for k in range(1, reps)]
        upper, bias_one = call(
            functools.partial(rep_join_kernel, giver),
            (jax.ShapeDtypeStruct((reps, piece, hidden_width), BF16), shape(8, hidden_width, F32)),
            (pltpu.VMEM((reps, BIAS_ROWS, hidden_width), BF16),),
        )(mine, *got)
    else:
        summed = lax.psum(own_half, ("feat", "rep"))
        upper, bias_two = summed[:half], summed[half : half + 1]
        bias_one = lax.psum(jnp.sum(blocks[0].astype(F32), 0, keepdims=True), "rep")
    panel = call(panel_sum_kernel, shape(share, hidden_width, BF16))(panels[0], *got_panel)

    panel_all = [panel] + [to_rep(panel, k) for k in range(1, reps)]
    grad_w1 = call(
        functools.partial(place_kernel, [functools.partial(giver, k) for k in range(reps)]),
        jax.ShapeDtypeStruct((reps, share, hidden_width), F32),
        (
            pltpu.VMEM((reps, share, hidden_width), F32),
            pltpu.SemaphoreType.DMA((reps,)),
        ),
        out_specs=pl.BlockSpec(memory_space=pltpu.HBM),
    )(*panel_all)
    grad_w1 = grad_w1.reshape(sets, width, hidden_width)
    if direct:
        upper_all = [upper] + [to_chip(upper, k) for k in range(1, chips)]
        upper_all = upper_all + [to_core(u) for u in upper_all]
        places = []
        for turn in range(cores):
            for k in range(chips):
                places.append(
                    lambda turn=turn, k=k: (
                        lax.bitwise_xor(core_of(), jnp.int32(turn)),
                        lax.bitwise_xor(chip_of(), jnp.int32(k)),
                    )
                )
        grad_w2, bias_one, bias_two = call(
            functools.partial(place_two_kernel, places),
            (
                jax.ShapeDtypeStruct((cores, reps, chips, piece, hidden_width), F32),
                jax.ShapeDtypeStruct((hidden_width,), F32),
                jax.ShapeDtypeStruct((hidden_width,), F32),
            ),
            (
                pltpu.VMEM((feat, reps, piece, hidden_width), F32),
                pltpu.SemaphoreType.DMA((feat + 2,)),
            ),
            out_specs=[pl.BlockSpec(memory_space=pltpu.HBM)] * 3,
        )(*upper_all, bias_one, bias_two)
    else:
        grad_w2, bias_one, bias_two = upper, bias_one[0], bias_two[0]
    grad_w2 = grad_w2.reshape(sets, hidden_width, hidden_width)
    return (grad_w1, bias_one, grad_w2, bias_two)


def solution(mesh):
    placed = (
        P("rep", None, "feat", None),
        P("rep", None, None, None, None),
        P("rep", "feat", None, None),
        P("rep", "feat", None, None, None),
        P(),
        P("rep", "feat", None, None),
    )
    return jax.shard_map(
        on_device,
        mesh=mesh,
        in_specs=placed,
        out_specs=(P(None, "feat", None), P(), P(), P()),
        check_vma=False,
    )
```

```python
import functools

import jax
import jax.numpy as jnp
from jax import lax
from jax.experimental import pallas as pl
from jax.experimental.pallas import tpu as pltpu
from jax.sharding import PartitionSpec as P


BITS = 16
BIAS_ROWS = 16
LOADED = range(6)
FIRST_SHARE = 5
F32 = jnp.float32
BF16 = jnp.bfloat16
NT = (((1,), (1,)), ((), ()))
TN = (((0,), (0,)), ((), ()))
VMEM = pl.BlockSpec(memory_space=pltpu.VMEM)


def dot(a, b, dims=(((1,), (0,)), ((), ()))):
    return lax.dot_general(a, b, dims, preferred_element_type=F32)


def reorder(rows):
    words = rows // BITS
    out = lax.broadcasted_iota(jnp.int32, (rows, rows), 0)
    src = lax.broadcasted_iota(jnp.int32, (rows, rows), 1)
    return jnp.where(src == BITS * (out % words) + out // words, 1.0, 0.0).astype(BF16)


def bits_two(words):
    count, cols = words.shape
    shifts = lax.broadcasted_iota(jnp.int32, (BITS, count, cols), 0)
    spread = jnp.bitwise_and(jnp.right_shift(words[None], shifts), 1)
    return spread.astype(F32).reshape(BITS * count, cols)


def split_rows(value):
    high = value.astype(BF16)
    return high.astype(F32), (value - high.astype(F32)).astype(BF16).astype(F32)


def pack_rows(*values):
    row = lax.broadcasted_iota(jnp.int32, (BIAS_ROWS, values[0].shape[1]), 0)
    packed = jnp.zeros(row.shape, F32)
    place = 0
    for value in values:
        for part in split_rows(value):
            packed = jnp.where(row == place, part, packed)
            place += 1
    return packed.astype(BF16)


def read_row(packed, place):
    rows = packed.astype(F32)
    return rows[2 * place : 2 * place + 1] + rows[2 * place + 1 : 2 * place + 2]


def upper_kernel(factor, core_of, *refs):
    count = len(LOADED)
    sources, (hidden_ref, own_ref, send_ref) = refs[:count], refs[count : count + 3]
    targets, (sums, sems) = refs[count + 5 : -2] + refs[count + 3 : count + 5], refs[-2:]
    weight_ref = targets[3]
    grad_ref, words_ref, pre_ref = targets[:3]
    copies = [
        pltpu.make_async_copy(source, target, sems.at[n])
        for n, (source, target) in enumerate(zip(sources, targets))
    ]
    for copy in copies:
        copy.start()
    for copy in copies[:3]:
        copy.wait()
    relations = words_ref.shape[0]
    seeds, width = grad_ref.shape
    scaled = grad_ref[...].astype(F32) * factor
    low = scaled.astype(BF16)
    low_bits = dot(reorder(seeds), low).astype(BF16)
    pre = pre_ref[...].astype(F32)
    hidden = jnp.maximum(pre, 0.0).astype(BF16)
    parts = sums.shape[0]
    rows = sums.shape[1]
    height = hidden.shape[1]
    per = rows // height
    sums[0, :height] = dot(hidden[:seeds], low, TN)
    matrices = []
    for r in range(1, relations + 1):
        spread = bits_two(words_ref[r - 1])
        inverse = 1.0 / jnp.maximum(jnp.sum(spread, axis=1, keepdims=True), 1.0)
        matrix = spread.astype(BF16)
        matrices.append((matrix, inverse))
        mixed = (dot(matrix, hidden) * inverse).astype(BF16)
        sums[r // per, (r % per) * height : (r % per + 1) * height] = dot(mixed, low_bits, TN)
    copies[3].wait()
    own = dot(low, weight_ref[0], NT)
    total = jnp.concatenate([own, jnp.zeros((pre.shape[0] - seeds, own.shape[1]), F32)], 0)
    for r, (matrix, inverse) in enumerate(matrices, 1):
        back = (dot(low_bits, weight_ref[r], NT) * inverse).astype(BF16)
        total = total + dot(matrix, back, TN)
    hidden_grad = jnp.where(pre > 0, total, 0.0).astype(BF16)
    hidden_ref[...] = dot(reorder(total.shape[0]), hidden_grad).astype(BF16)
    core = core_of()
    own_ref[:rows] = sums[core]
    other = 0 if parts == 1 else 1 - core
    send_ref[:rows] = sums[other]
    bias = jnp.sum(scaled, 0, keepdims=True)
    own_ref[rows:] = jnp.broadcast_to(bias, (BIAS_ROWS, width))
    send_ref[rows:] = jnp.broadcast_to(bias, (BIAS_ROWS, width))
    for copy in copies[4:]:
        copy.wait()


def pair_kernel(taker, own_ref, got_ref, *refs):
    outs, sums = refs[:-1], refs[-1]
    reps, rows, width = sums.shape
    height = reps * rows
    total = own_ref[:height] + got_ref[:height]
    sums[...] = total.reshape(reps, rows, width)
    bias = own_ref[height:] + got_ref[height:]
    packed = pack_rows(bias[0:1])
    outs[0][:rows] = sums[taker(0)]
    outs[0][rows:] = packed.astype(F32)
    for k in range(1, reps):
        outs[k][:rows] = sums[taker(k)].astype(BF16)
        outs[k][rows:] = packed


def rep_sum_kernel(giver, chip_of, own_ref, *refs):
    reps, chips = refs[-1].shape[0], refs[-2].shape[0]
    got, outs, (sums, slots) = refs[: reps - 1], refs[reps - 1 : -2], refs[-2:]
    rows = sums.shape[1]
    height = chips * rows
    total = own_ref[:height]
    slots[giver(0)] = own_ref[height:]
    for k, piece in enumerate(got, 1):
        total = total + piece[:height].astype(F32)
        slots[giver(k)] = piece[height:].astype(F32)
    sums[...] = total.reshape(sums.shape)
    bias = read_row(slots[0], 0)
    for j in range(1, reps):
        bias = bias + read_row(slots[j], 0)
    packed = pack_rows(bias)
    chip = chip_of()
    outs[0][:rows] = sums[chip]
    outs[0][rows:] = packed.astype(F32)
    for k in range(1, chips):
        outs[k][:rows] = sums[lax.bitwise_xor(chip, k)].astype(BF16)
        outs[k][rows:] = packed


def gather_kernel(first, count, column_ref, word_ref, out_ref, wide):
    width, nodes = column_ref.shape[1:]
    relations, words = word_ref.shape[1:3]
    rows = words * BITS
    select = reorder(rows)
    wide[width:] = jnp.ones((wide.shape[0] - width, nodes), BF16)
    bit = lax.broadcasted_iota(jnp.int32, (1, rows), 1) // words
    power = lax.shift_left(jnp.int32(1), BITS - 1 - bit).astype(F32) * 2.0 ** (1 - BITS)

    def batch(b):
        column = column_ref[first + b]
        wide[:width] = column
        place = pl.ds(pl.multiple_of(b * rows, rows), rows)
        out_ref[:width, place] = dot(column[:, :rows], select, NT).astype(BF16)
        for r in range(relations):
            word = word_ref[first + b, r]
            matrix = jnp.concatenate(
                [jnp.bitwise_and(word, 1 << k).astype(F32).astype(BF16) for k in range(BITS)], 0
            )
            value = dot(wide[...], matrix, NT)
            total = value[width : width + 1] * power
            scale = power / jnp.maximum(total, 1.0)
            out_ref[(r + 1) * width : (r + 2) * width, place] = (value[:width] * scale).astype(BF16)

    if count <= 8:
        for b in range(count):
            batch(b)
    else:
        lax.fori_loop(0, count, lambda b, unused: (batch(b), unused)[1], 0)


def panel_kernel(taker, order, parts, *refs):
    gathered, refs = refs[:parts], refs[parts:]
    blocks, (own_ref, *outs) = refs[: len(order)], refs[len(order) : -2]
    stack, sums = refs[-2:]
    height = blocks[0].shape[0]
    for block, place in zip(blocks, order):
        start = pl.multiple_of(place() * height, height)
        stack[pl.ds(start, height)] = block[...]
    total, place = None, 0
    for part in gathered:
        deep = part.shape[1]
        value = dot(part[...], stack[place : place + deep])
        total = value if total is None else total + value
        place += deep
    sums[...] = total.reshape(sums.shape)
    reps = sums.shape[0]
    own_ref[...] = sums[taker(0)]
    for k in range(1, reps):
        outs[k - 1][...] = sums[taker(k)].astype(BF16)


def call(body, outs, scratch=(), flops=1000000, vmem=8, **keys):
    return pl.pallas_call(
        body,
        out_shape=outs,
        scratch_shapes=list(scratch),
        compiler_params=pltpu.CompilerParams(vmem_limit_bytes=vmem * 1024 * 1024),
        cost_estimate=pl.CostEstimate(flops=flops, bytes_accessed=1000000, transcendentals=0),
        **keys,
    )


def shape(rows, cols, dtype):
    return jax.ShapeDtypeStruct((rows, cols), dtype)


def plane_sum_kernel(chip_of, order, own_ref, *refs):
    blocks, got = refs[: len(order)], refs[len(order) : -4]
    out, two_ref, slots, rows_sum = refs[-4:]
    rows = out.shape[0] - BIAS_ROWS
    chip = chip_of()
    total = own_ref[:rows]
    slots[chip] = own_ref[rows:]
    for k, piece in enumerate(got, 1):
        total = total + piece[:rows].astype(F32)
        slots[lax.bitwise_xor(chip, k)] = piece[rows:].astype(F32)
    out[:rows] = total.astype(BF16)
    two = read_row(slots[0], 0)
    for j in range(1, slots.shape[0]):
        two = two + read_row(slots[j], 0)
    two_ref[...] = jnp.broadcast_to(two, two_ref.shape)
    for block, place in zip(blocks, order):
        rows_sum[place()] = jnp.sum(block[...].astype(F32), 0, keepdims=True)
    one = rows_sum[0]
    for j in range(1, len(order)):
        one = one + rows_sum[j]
    out[rows:] = pack_rows(one)


def rep_join_kernel(giver, *refs):
    parts, (out, one_ref, slots) = refs[:-3], refs[-3:]
    rows = out.shape[1]
    for k, part in enumerate(parts):
        out[giver(k)] = part[:rows]
        slots[giver(k)] = part[rows:]
    one = read_row(slots[0], 0)
    for j in range(1, len(parts)):
        one = one + read_row(slots[j], 0)
    one_ref[...] = jnp.broadcast_to(one, one_ref.shape)


def panel_sum_kernel(own_ref, *refs):
    total = own_ref[...]
    for piece in refs[:-1]:
        total = total + piece[...].astype(F32)
    refs[-1][...] = total.astype(BF16)


def place_kernel(order, *refs):
    blocks, (out, held, sems) = refs[:-3], refs[-3:]
    copies = []
    for n, (block, place) in enumerate(zip(blocks, order)):
        held[n] = block[...].astype(F32)
        copies.append(pltpu.make_async_copy(held.at[n], out.at[place()], sems.at[n]))
        copies[-1].start()
    for copy in copies:
        copy.wait()


def place_two_kernel(order, *refs):
    blocks, (one_ref, two_ref) = refs[: len(order)], refs[len(order) : len(order) + 2]
    out, one_out, two_out, held, sems = refs[len(order) + 2 :]
    copies = [
        pltpu.make_async_copy(one_ref.at[0], one_out, sems.at[len(order)]),
        pltpu.make_async_copy(two_ref.at[0], two_out, sems.at[len(order) + 1]),
    ]
    for copy in copies:
        copy.start()
    for n, (block, place) in enumerate(zip(blocks, order)):
        core, chip = place()
        held[n] = block[...].astype(F32)
        copies.append(pltpu.make_async_copy(held.at[n], out.at[core, :, chip], sems.at[n]))
        copies[-1].start()
    for copy in copies:
        copy.wait()


def on_device(features, adjacency_one, pre_hidden, adjacency_two, weight_two, out_grad):
    feat = lax.axis_size("feat")
    reps = lax.axis_size("rep")
    pre, words_two, grad = pre_hidden[0, 0], adjacency_two[0, 0], out_grad[0, 0]
    columns, words_one = features[0], adjacency_one[0]
    batches, width, nodes = columns.shape
    relations, words = words_one.shape[1:3]
    rows_one = words * BITS
    hidden_rows, hidden_width = pre.shape
    seeds = grad.shape[0]
    factor = float(seeds * feat * reps) ** (-0.5)
    sets = relations + 1
    cores = 2
    chips = feat // cores
    direct = feat <= 8 and feat % cores == 0 and chips & (chips - 1) == 0
    direct = direct and sets * hidden_width % (8 * feat * reps) == 0

    def core_of():
        return lax.axis_index("feat") % cores

    def chip_of():
        return lax.axis_index("feat") // cores

    def in_hbm(value):
        return pltpu.with_memory_space_constraint(value, pltpu.HBM)

    loaded = (grad, words_two, pre, weight_two, words_one, columns)
    upper_rows = sets * hidden_width
    half = upper_rows // cores if direct else upper_rows
    kept = (words_one, columns)
    hidden, own_half, send_half, words_one, columns = call(
        functools.partial(upper_kernel, factor, core_of if direct else lambda: 0),
        (shape(hidden_rows, hidden_width, BF16),)
        + (shape(half + BIAS_ROWS, hidden_width, F32),) * 2
        + tuple(jax.ShapeDtypeStruct(v.shape, v.dtype) for v in kept),
        [pltpu.VMEM(v.shape, v.dtype) for v in loaded[:4]]
        + [
            pltpu.VMEM((upper_rows // half, half, hidden_width), F32),
            pltpu.SemaphoreType.DMA((len(loaded),)),
        ],
        vmem=8 + sum(v.size * v.dtype.itemsize for v in loaded) // 2**20,
        in_specs=[pl.BlockSpec(memory_space=pltpu.HBM)] * len(loaded),
    )(*map(in_hbm, loaded))

    first = batches * FIRST_SHARE // 8
    runs = [(0, first), (first, batches - first)]
    gathered = []
    for start, run in runs:
        gathered.append(
            call(
                functools.partial(gather_kernel, start, run),
                shape(sets * width, run * rows_one, BF16),
                (pltpu.VMEM((width + 16, nodes), BF16),),
                flops=3000000000,
                vmem=12 + 2 * words_one.size * 4 // 2**20,
            )(columns, words_one)
        )

    def to_chip(value, k):
        pairs = [(i, (i // cores ^ k) * cores + i % cores) for i in range(feat)]
        return lax.ppermute(value, "feat", pairs)

    def to_core(value):
        return lax.ppermute(value, "feat", [(i, i ^ 1) for i in range(feat)])

    flip = reps & (reps - 1) == 0

    def giver(k):
        rep = lax.axis_index("rep")
        return lax.bitwise_xor(rep, jnp.int32(k)) if flip else (rep + reps - k) % reps

    def taker(k):
        rep = lax.axis_index("rep")
        return lax.bitwise_xor(rep, jnp.int32(k)) if flip else (rep + k) % reps

    def to_rep(value, k):
        pairs = [(i, (i ^ k) if flip else (i + k) % reps) for i in range(reps)]
        return lax.ppermute(value, "rep", pairs)

    piece = half // (chips * reps)
    share = sets * width // reps

    if direct:
        blocks = [hidden] + [to_chip(hidden, k) for k in range(1, chips)]
        blocks = blocks + [to_core(block) for block in blocks]
        order = []
        for turn in range(cores):
            for k in range(chips):
                order.append(
                    lambda turn=turn, k=k: lax.bitwise_xor(
                        lax.axis_index("feat"), jnp.int32(k * cores + turn)
                    )
                )
        got_half = to_core(send_half)
        tall = half // reps + BIAS_ROWS
        thirds = call(
            functools.partial(pair_kernel, taker),
            (shape(tall, hidden_width, F32),) + (shape(tall, hidden_width, BF16),) * (reps - 1),
            (pltpu.VMEM((reps, half // reps, hidden_width), F32),),
        )(own_half, got_half)
        got = [to_rep(thirds[k], k) for k in range(1, reps)]
        tall = piece + BIAS_ROWS
        pieces = call(
            functools.partial(rep_sum_kernel, giver, chip_of),
            (shape(tall, hidden_width, F32),) + (shape(tall, hidden_width, BF16),) * (chips - 1),
            (
                pltpu.VMEM((chips, piece, hidden_width), F32),
                pltpu.VMEM((reps, BIAS_ROWS, hidden_width), F32),
            ),
        )(thirds[0], *got)
        got = [to_chip(pieces[k], k) for k in range(1, chips)]
    else:
        blocks = [lax.all_gather(hidden, "feat", axis=0, tiled=True)]
        order = [lambda: 0]

    stack_bytes = batches * rows_one * (hidden_width + sets * width) * 2
    panels = call(
        functools.partial(panel_kernel, taker, order, len(runs)),
        (shape(share, hidden_width, F32),) + (shape(share, hidden_width, BF16),) * (reps - 1),
        (
            pltpu.VMEM((batches * rows_one, hidden_width), BF16),
            pltpu.VMEM((reps, share, hidden_width), F32),
        ),
        vmem=8 + 2 * stack_bytes // 2**20,
    )(*gathered, *blocks)
    got_panel = [to_rep(panels[k], k) for k in range(1, reps)]
    if direct:
        mine, bias_two = call(
            functools.partial(plane_sum_kernel, chip_of, order),
            (shape(tall, hidden_width, BF16), shape(8, hidden_width, F32)),
            (
                pltpu.VMEM((chips, BIAS_ROWS, hidden_width), F32),
                pltpu.VMEM((feat, 1, hidden_width), F32),
            ),
        )(pieces[0], *blocks, *got)
        got = [to_rep(mine, k) for k in range(1, reps)]
        upper, bias_one = call(
            functools.partial(rep_join_kernel, giver),
            (jax.ShapeDtypeStruct((reps, piece, hidden_width), BF16), shape(8, hidden_width, F32)),
            (pltpu.VMEM((reps, BIAS_ROWS, hidden_width), BF16),),
        )(mine, *got)
    else:
        summed = lax.psum(own_half, ("feat", "rep"))
        upper, bias_two = summed[:half], summed[half : half + 1]
        bias_one = lax.psum(jnp.sum(blocks[0].astype(F32), 0, keepdims=True), "rep")
    panel = call(panel_sum_kernel, shape(share, hidden_width, BF16))(panels[0], *got_panel)

    panel_all = [panel] + [to_rep(panel, k) for k in range(1, reps)]
    grad_w1 = call(
        functools.partial(place_kernel, [functools.partial(giver, k) for k in range(reps)]),
        jax.ShapeDtypeStruct((reps, share, hidden_width), F32),
        (
            pltpu.VMEM((reps, share, hidden_width), F32),
            pltpu.SemaphoreType.DMA((reps,)),
        ),
        out_specs=pl.BlockSpec(memory_space=pltpu.HBM),
    )(*panel_all)
    grad_w1 = grad_w1.reshape(sets, width, hidden_width)
    if direct:
        upper_all = [upper] + [to_chip(upper, k) for k in range(1, chips)]
        upper_all = upper_all + [to_core(u) for u in upper_all]
        places = []
        for turn in range(cores):
            for k in range(chips):
                places.append(
                    lambda turn=turn, k=k: (
                        lax.bitwise_xor(core_of(), jnp.int32(turn)),
                        lax.bitwise_xor(chip_of(), jnp.int32(k)),
                    )
                )
        grad_w2, bias_one, bias_two = call(
            functools.partial(place_two_kernel, places),
            (
                jax.ShapeDtypeStruct((cores, reps, chips, piece, hidden_width), F32),
                jax.ShapeDtypeStruct((hidden_width,), F32),
                jax.ShapeDtypeStruct((hidden_width,), F32),
            ),
            (
                pltpu.VMEM((feat, reps, piece, hidden_width), F32),
                pltpu.SemaphoreType.DMA((feat + 2,)),
            ),
            out_specs=[pl.BlockSpec(memory_space=pltpu.HBM)] * 3,
        )(*upper_all, bias_one, bias_two)
    else:
        grad_w2, bias_one, bias_two = upper, bias_one[0], bias_two[0]
    grad_w2 = grad_w2.reshape(sets, hidden_width, hidden_width)
    return (grad_w1, bias_one, grad_w2, bias_two)


def solution(mesh):
    placed = (
        P("rep", None, "feat", None),
        P("rep", None, None, None, None),
        P("rep", "feat", None, None),
        P("rep", "feat", None, None, None),
        P(),
        P("rep", "feat", None, None),
    )
    return jax.shard_map(
        on_device,
        mesh=mesh,
        in_specs=placed,
        out_specs=(P(None, "feat", None), P(), P(), P()),
        check_vma=False,
    )
```

```python
import functools

import jax
import jax.numpy as jnp
from jax import lax
from jax.experimental import pallas as pl
from jax.experimental.pallas import tpu as pltpu
from jax.sharding import PartitionSpec as P


BITS = 16
BIAS_ROWS = 16
LOADED = range(6)
FIRST_SHARE = 5
F32 = jnp.float32
BF16 = jnp.bfloat16
NT = (((1,), (1,)), ((), ()))
TN = (((0,), (0,)), ((), ()))
VMEM = pl.BlockSpec(memory_space=pltpu.VMEM)


def dot(a, b, dims=(((1,), (0,)), ((), ()))):
    return lax.dot_general(a, b, dims, preferred_element_type=F32)


def reorder(rows):
    words = rows // BITS
    out = lax.broadcasted_iota(jnp.int32, (rows, rows), 0)
    src = lax.broadcasted_iota(jnp.int32, (rows, rows), 1)
    return jnp.where(src == BITS * (out % words) + out // words, 1.0, 0.0).astype(BF16)


def bits_two(words):
    count, cols = words.shape
    shifts = lax.broadcasted_iota(jnp.int32, (BITS, count, cols), 0)
    spread = jnp.bitwise_and(jnp.right_shift(words[None], shifts), 1)
    return spread.astype(F32).reshape(BITS * count, cols)


def split_rows(value):
    high = value.astype(BF16)
    return high.astype(F32), (value - high.astype(F32)).astype(BF16).astype(F32)


def pack_rows(*values):
    row = lax.broadcasted_iota(jnp.int32, (BIAS_ROWS, values[0].shape[1]), 0)
    packed = jnp.zeros(row.shape, F32)
    place = 0
    for value in values:
        for part in split_rows(value):
            packed = jnp.where(row == place, part, packed)
            place += 1
    return packed.astype(BF16)


def read_row(packed, place):
    rows = packed.astype(F32)
    return rows[2 * place : 2 * place + 1] + rows[2 * place + 1 : 2 * place + 2]


def upper_kernel(factor, core_of, *refs):
    count = len(LOADED)
    sources, (hidden_ref, own_ref, send_ref) = refs[:count], refs[count : count + 3]
    targets, (sums, sems) = refs[count + 5 : -2] + refs[count + 3 : count + 5], refs[-2:]
    weight_ref = targets[3]
    grad_ref, words_ref, pre_ref = targets[:3]
    copies = [
        pltpu.make_async_copy(source, target, sems.at[n])
        for n, (source, target) in enumerate(zip(sources, targets))
    ]
    for copy in copies:
        copy.start()
    for copy in copies[:3]:
        copy.wait()
    relations = words_ref.shape[0]
    seeds, width = grad_ref.shape
    scaled = grad_ref[...].astype(F32) * factor
    low = scaled.astype(BF16)
    low_bits = dot(reorder(seeds), low).astype(BF16)
    pre = pre_ref[...].astype(F32)
    hidden = jnp.maximum(pre, 0.0).astype(BF16)
    parts = sums.shape[0]
    rows = sums.shape[1]
    height = hidden.shape[1]
    per = rows // height
    sums[0, :height] = dot(hidden[:seeds], low, TN)
    matrices = []
    for r in range(1, relations + 1):
        spread = bits_two(words_ref[r - 1])
        inverse = 1.0 / jnp.maximum(jnp.sum(spread, axis=1, keepdims=True), 1.0)
        matrix = spread.astype(BF16)
        matrices.append((matrix, inverse))
        mixed = (dot(matrix, hidden) * inverse).astype(BF16)
        sums[r // per, (r % per) * height : (r % per + 1) * height] = dot(mixed, low_bits, TN)
    copies[3].wait()
    own = dot(low, weight_ref[0], NT)
    total = jnp.concatenate([own, jnp.zeros((pre.shape[0] - seeds, own.shape[1]), F32)], 0)
    for r, (matrix, inverse) in enumerate(matrices, 1):
        back = (dot(low_bits, weight_ref[r], NT) * inverse).astype(BF16)
        total = total + dot(matrix, back, TN)
    hidden_grad = jnp.where(pre > 0, total, 0.0).astype(BF16)
    hidden_ref[...] = dot(reorder(total.shape[0]), hidden_grad).astype(BF16)
    core = core_of()
    own_ref[:rows] = sums[core]
    other = 0 if parts == 1 else 1 - core
    send_ref[:rows] = sums[other]
    bias = jnp.sum(scaled, 0, keepdims=True)
    own_ref[rows:] = jnp.broadcast_to(bias, (BIAS_ROWS, width))
    send_ref[rows:] = jnp.broadcast_to(bias, (BIAS_ROWS, width))
    for copy in copies[4:]:
        copy.wait()


def pair_kernel(taker, own_ref, got_ref, *refs):
    outs, sums = refs[:-1], refs[-1]
    reps, rows, width = sums.shape
    height = reps * rows
    total = own_ref[:height] + got_ref[:height]
    sums[...] = total.reshape(reps, rows, width)
    bias = own_ref[height:] + got_ref[height:]
    packed = pack_rows(bias[0:1])
    outs[0][:rows] = sums[taker(0)]
    outs[0][rows:] = packed.astype(F32)
    for k in range(1, reps):
        outs[k][:rows] = sums[taker(k)].astype(BF16)
        outs[k][rows:] = packed


def rep_sum_kernel(giver, chip_of, own_ref, *refs):
    reps, chips = refs[-1].shape[0], refs[-2].shape[0]
    got, outs, (sums, slots) = refs[: reps - 1], refs[reps - 1 : -2], refs[-2:]
    rows = sums.shape[1]
    height = chips * rows
    total = own_ref[:height]
    slots[giver(0)] = own_ref[height:]
    for k, piece in enumerate(got, 1):
        total = total + piece[:height].astype(F32)
        slots[giver(k)] = piece[height:].astype(F32)
    sums[...] = total.reshape(sums.shape)
    bias = read_row(slots[0], 0)
    for j in range(1, reps):
        bias = bias + read_row(slots[j], 0)
    packed = pack_rows(bias)
    chip = chip_of()
    outs[0][:rows] = sums[chip]
    outs[0][rows:] = packed.astype(F32)
    for k in range(1, chips):
        outs[k][:rows] = sums[lax.bitwise_xor(chip, k)].astype(BF16)
        outs[k][rows:] = packed


def gather_kernel(first, count, column_ref, word_ref, out_ref, wide):
    width, nodes = column_ref.shape[1:]
    relations, words = word_ref.shape[1:3]
    rows = words * BITS
    select = reorder(rows)
    wide[width:] = jnp.ones((wide.shape[0] - width, nodes), BF16)
    bit = lax.broadcasted_iota(jnp.int32, (1, rows), 1) // words
    power = lax.shift_left(jnp.int32(1), BITS - 1 - bit).astype(F32) * 2.0 ** (1 - BITS)

    def batch(b):
        column = column_ref[first + b]
        wide[:width] = column
        place = pl.ds(pl.multiple_of(b * rows, rows), rows)
        out_ref[:width, place] = dot(column[:, :rows], select, NT).astype(BF16)
        for r in range(relations):
            word = word_ref[first + b, r]
            matrix = jnp.concatenate(
                [jnp.bitwise_and(word, 1 << k).astype(F32).astype(BF16) for k in range(BITS)], 0
            )
            value = dot(wide[...], matrix, NT)
            total = value[width : width + 1] * power
            scale = power / jnp.maximum(total, 1.0)
            out_ref[(r + 1) * width : (r + 2) * width, place] = (value[:width] * scale).astype(BF16)

    if count <= 8:
        for b in range(count):
            batch(b)
    else:
        lax.fori_loop(0, count, lambda b, unused: (batch(b), unused)[1], 0)


def panel_kernel(taker, order, parts, *refs):
    gathered, refs = refs[:parts], refs[parts:]
    blocks, (own_ref, *outs) = refs[: len(order)], refs[len(order) : -2]
    stack, sums = refs[-2:]
    height = blocks[0].shape[0]
    for block, place in zip(blocks, order):
        start = pl.multiple_of(place() * height, height)
        stack[pl.ds(start, height)] = block[...]
    total, place = None, 0
    for part in gathered:
        deep = part.shape[1]
        value = dot(part[...], stack[place : place + deep])
        total = value if total is None else total + value
        place += deep
    sums[...] = total.reshape(sums.shape)
    reps = sums.shape[0]
    own_ref[...] = sums[taker(0)]
    for k in range(1, reps):
        outs[k - 1][...] = sums[taker(k)].astype(BF16)


def call(body, outs, scratch=(), flops=1000000, vmem=8, **keys):
    return pl.pallas_call(
        body,
        out_shape=outs,
        scratch_shapes=list(scratch),
        compiler_params=pltpu.CompilerParams(vmem_limit_bytes=vmem * 1024 * 1024),
        cost_estimate=pl.CostEstimate(flops=flops, bytes_accessed=1000000, transcendentals=0),
        **keys,
    )


def shape(rows, cols, dtype):
    return jax.ShapeDtypeStruct((rows, cols), dtype)


def plane_sum_kernel(chip_of, order, own_ref, *refs):
    blocks, got = refs[: len(order)], refs[len(order) : -4]
    out, two_ref, slots, rows_sum = refs[-4:]
    rows = out.shape[0] - BIAS_ROWS
    chip = chip_of()
    total = own_ref[:rows]
    slots[chip] = own_ref[rows:]
    for k, piece in enumerate(got, 1):
        total = total + piece[:rows].astype(F32)
        slots[lax.bitwise_xor(chip, k)] = piece[rows:].astype(F32)
    out[:rows] = total.astype(BF16)
    two = read_row(slots[0], 0)
    for j in range(1, slots.shape[0]):
        two = two + read_row(slots[j], 0)
    two_ref[...] = jnp.broadcast_to(two, two_ref.shape)
    for block, place in zip(blocks, order):
        rows_sum[place()] = jnp.sum(block[...].astype(F32), 0, keepdims=True)
    one = rows_sum[0]
    for j in range(1, len(order)):
        one = one + rows_sum[j]
    out[rows:] = pack_rows(one)


def rep_join_kernel(giver, *refs):
    parts, (out, one_ref, slots) = refs[:-3], refs[-3:]
    rows = out.shape[1]
    for k, part in enumerate(parts):
        out[giver(k)] = part[:rows]
        slots[giver(k)] = part[rows:]
    one = read_row(slots[0], 0)
    for j in range(1, len(parts)):
        one = one + read_row(slots[j], 0)
    one_ref[...] = jnp.broadcast_to(one, one_ref.shape)


def panel_sum_kernel(own_ref, *refs):
    total = own_ref[...]
    for piece in refs[:-1]:
        total = total + piece[...].astype(F32)
    refs[-1][...] = total.astype(BF16)


def place_kernel(order, *refs):
    blocks, (out, held, sems) = refs[:-3], refs[-3:]
    copies = []
    for n, (block, place) in enumerate(zip(blocks, order)):
        held[n] = block[...].astype(F32)
        copies.append(pltpu.make_async_copy(held.at[n], out.at[place()], sems.at[n]))
        copies[-1].start()
    for copy in copies:
        copy.wait()


def place_blocks(blocks, order, out, held, sems):
    copies = []
    for n, (block, place) in enumerate(zip(blocks, order)):
        core, chip = place()
        held[n] = block[...].astype(F32)
        copies.append(pltpu.make_async_copy(held.at[n], out.at[core, :, chip], sems.at[n]))
        copies[-1].start()
    return copies


def place_first_kernel(order, *refs):
    blocks, (one_ref, two_ref) = refs[: len(order)], refs[len(order) : len(order) + 2]
    out, one_out, two_out, held, sems = refs[len(order) + 2 :]
    copies = [
        pltpu.make_async_copy(one_ref.at[0], one_out, sems.at[len(order)]),
        pltpu.make_async_copy(two_ref.at[0], two_out, sems.at[len(order) + 1]),
    ]
    for copy in copies:
        copy.start()
    copies += place_blocks(blocks, order, out, held, sems)
    for copy in copies:
        copy.wait()


def place_rest_kernel(order, begun, *refs):
    blocks, (out, held, sems) = refs[: len(order)], refs[len(order) :]
    for copy in place_blocks(blocks, order, out, held, sems):
        copy.wait()


def on_device(features, adjacency_one, pre_hidden, adjacency_two, weight_two, out_grad):
    feat = lax.axis_size("feat")
    reps = lax.axis_size("rep")
    pre, words_two, grad = pre_hidden[0, 0], adjacency_two[0, 0], out_grad[0, 0]
    columns, words_one = features[0], adjacency_one[0]
    batches, width, nodes = columns.shape
    relations, words = words_one.shape[1:3]
    rows_one = words * BITS
    hidden_rows, hidden_width = pre.shape
    seeds = grad.shape[0]
    factor = float(seeds * feat * reps) ** (-0.5)
    sets = relations + 1
    cores = 2
    chips = feat // cores
    direct = feat <= 8 and feat % cores == 0 and chips & (chips - 1) == 0
    direct = direct and sets * hidden_width % (8 * feat * reps) == 0

    def core_of():
        return lax.axis_index("feat") % cores

    def chip_of():
        return lax.axis_index("feat") // cores

    def in_hbm(value):
        return pltpu.with_memory_space_constraint(value, pltpu.HBM)

    loaded = (grad, words_two, pre, weight_two, words_one, columns)
    upper_rows = sets * hidden_width
    half = upper_rows // cores if direct else upper_rows
    kept = (words_one, columns)
    hidden, own_half, send_half, words_one, columns = call(
        functools.partial(upper_kernel, factor, core_of if direct else lambda: 0),
        (shape(hidden_rows, hidden_width, BF16),)
        + (shape(half + BIAS_ROWS, hidden_width, F32),) * 2
        + tuple(jax.ShapeDtypeStruct(v.shape, v.dtype) for v in kept),
        [pltpu.VMEM(v.shape, v.dtype) for v in loaded[:4]]
        + [
            pltpu.VMEM((upper_rows // half, half, hidden_width), F32),
            pltpu.SemaphoreType.DMA((len(loaded),)),
        ],
        vmem=8 + sum(v.size * v.dtype.itemsize for v in loaded) // 2**20,
        in_specs=[pl.BlockSpec(memory_space=pltpu.HBM)] * len(loaded),
    )(*map(in_hbm, loaded))

    first = batches * FIRST_SHARE // 8
    runs = [(0, first), (first, batches - first)]
    gathered = []
    for start, run in runs:
        gathered.append(
            call(
                functools.partial(gather_kernel, start, run),
                shape(sets * width, run * rows_one, BF16),
                (pltpu.VMEM((width + 16, nodes), BF16),),
                flops=3000000000,
                vmem=12 + 2 * words_one.size * 4 // 2**20,
            )(columns, words_one)
        )

    def to_chip(value, k):
        pairs = [(i, (i // cores ^ k) * cores + i % cores) for i in range(feat)]
        return lax.ppermute(value, "feat", pairs)

    def to_core(value):
        return lax.ppermute(value, "feat", [(i, i ^ 1) for i in range(feat)])

    flip = reps & (reps - 1) == 0

    def giver(k):
        rep = lax.axis_index("rep")
        return lax.bitwise_xor(rep, jnp.int32(k)) if flip else (rep + reps - k) % reps

    def taker(k):
        rep = lax.axis_index("rep")
        return lax.bitwise_xor(rep, jnp.int32(k)) if flip else (rep + k) % reps

    def to_rep(value, k):
        pairs = [(i, (i ^ k) if flip else (i + k) % reps) for i in range(reps)]
        return lax.ppermute(value, "rep", pairs)

    piece = half // (chips * reps)
    share = sets * width // reps

    if direct:
        blocks = [hidden] + [to_chip(hidden, k) for k in range(1, chips)]
        blocks = blocks + [to_core(block) for block in blocks]
        order = []
        for turn in range(cores):
            for k in range(chips):
                order.append(
                    lambda turn=turn, k=k: lax.bitwise_xor(
                        lax.axis_index("feat"), jnp.int32(k * cores + turn)
                    )
                )
        got_half = to_core(send_half)
        tall = half // reps + BIAS_ROWS
        thirds = call(
            functools.partial(pair_kernel, taker),
            (shape(tall, hidden_width, F32),) + (shape(tall, hidden_width, BF16),) * (reps - 1),
            (pltpu.VMEM((reps, half // reps, hidden_width), F32),),
        )(own_half, got_half)
        got = [to_rep(thirds[k], k) for k in range(1, reps)]
        tall = piece + BIAS_ROWS
        pieces = call(
            functools.partial(rep_sum_kernel, giver, chip_of),
            (shape(tall, hidden_width, F32),) + (shape(tall, hidden_width, BF16),) * (chips - 1),
            (
                pltpu.VMEM((chips, piece, hidden_width), F32),
                pltpu.VMEM((reps, BIAS_ROWS, hidden_width), F32),
            ),
        )(thirds[0], *got)
        got = [to_chip(pieces[k], k) for k in range(1, chips)]
    else:
        blocks = [lax.all_gather(hidden, "feat", axis=0, tiled=True)]
        order = [lambda: 0]

    stack_bytes = batches * rows_one * (hidden_width + sets * width) * 2
    panels = call(
        functools.partial(panel_kernel, taker, order, len(runs)),
        (shape(share, hidden_width, F32),) + (shape(share, hidden_width, BF16),) * (reps - 1),
        (
            pltpu.VMEM((batches * rows_one, hidden_width), BF16),
            pltpu.VMEM((reps, share, hidden_width), F32),
        ),
        vmem=8 + 2 * stack_bytes // 2**20,
    )(*gathered, *blocks)
    got_panel = [to_rep(panels[k], k) for k in range(1, reps)]
    if direct:
        mine, bias_two = call(
            functools.partial(plane_sum_kernel, chip_of, order),
            (shape(tall, hidden_width, BF16), shape(8, hidden_width, F32)),
            (
                pltpu.VMEM((chips, BIAS_ROWS, hidden_width), F32),
                pltpu.VMEM((feat, 1, hidden_width), F32),
            ),
        )(pieces[0], *blocks, *got)
        got = [to_rep(mine, k) for k in range(1, reps)]
        upper, bias_one = call(
            functools.partial(rep_join_kernel, giver),
            (jax.ShapeDtypeStruct((reps, piece, hidden_width), BF16), shape(8, hidden_width, F32)),
            (pltpu.VMEM((reps, BIAS_ROWS, hidden_width), BF16),),
        )(mine, *got)
    else:
        summed = lax.psum(own_half, ("feat", "rep"))
        upper, bias_two = summed[:half], summed[half : half + 1]
        bias_one = lax.psum(jnp.sum(blocks[0].astype(F32), 0, keepdims=True), "rep")
    panel = call(panel_sum_kernel, shape(share, hidden_width, BF16))(panels[0], *got_panel)

    panel_all = [panel] + [to_rep(panel, k) for k in range(1, reps)]
    grad_w1 = call(
        functools.partial(place_kernel, [functools.partial(giver, k) for k in range(reps)]),
        jax.ShapeDtypeStruct((reps, share, hidden_width), F32),
        (
            pltpu.VMEM((reps, share, hidden_width), F32),
            pltpu.SemaphoreType.DMA((reps,)),
        ),
        out_specs=pl.BlockSpec(memory_space=pltpu.HBM),
    )(*panel_all)
    grad_w1 = grad_w1.reshape(sets, width, hidden_width)
    if direct:
        upper_all = [upper] + [to_chip(upper, k) for k in range(1, chips)]
        upper_all = upper_all + [to_core(u) for u in upper_all]
        places = []
        for turn in range(cores):
            for k in range(chips):
                places.append(
                    lambda turn=turn, k=k: (
                        lax.bitwise_xor(core_of(), jnp.int32(turn)),
                        lax.bitwise_xor(chip_of(), jnp.int32(k)),
                    )
                )
        early = [n * chips for n in range(cores)]
        late = [n for n in range(feat) if n not in early]
        whole = jax.ShapeDtypeStruct((cores, reps, chips, piece, hidden_width), F32)
        in_memory = pl.BlockSpec(memory_space=pltpu.HBM)
        begun, bias_one, bias_two = call(
            functools.partial(place_first_kernel, [places[n] for n in early]),
            (whole,) + (jax.ShapeDtypeStruct((hidden_width,), F32),) * 2,
            (
                pltpu.VMEM((len(early), reps, piece, hidden_width), F32),
                pltpu.SemaphoreType.DMA((len(early) + 2,)),
            ),
            out_specs=[in_memory] * 3,
        )(*[upper_all[n] for n in early], bias_one, bias_two)
        grad_w2 = call(
            functools.partial(place_rest_kernel, [places[n] for n in late]),
            whole,
            (
                pltpu.VMEM((len(late), reps, piece, hidden_width), F32),
                pltpu.SemaphoreType.DMA((len(late),)),
            ),
            in_specs=[in_memory] + [VMEM] * len(late),
            out_specs=in_memory,
            input_output_aliases={0: 0},
        )(begun, *[upper_all[n] for n in late])
    else:
        grad_w2, bias_one, bias_two = upper, bias_one[0], bias_two[0]
    grad_w2 = grad_w2.reshape(sets, hidden_width, hidden_width)
    return (grad_w1, bias_one, grad_w2, bias_two)


def solution(mesh):
    placed = (
        P("rep", None, "feat", None),
        P("rep", None, None, None, None),
        P("rep", "feat", None, None),
        P("rep", "feat", None, None, None),
        P(),
        P("rep", "feat", None, None),
    )
    return jax.shard_map(
        on_device,
        mesh=mesh,
        in_specs=placed,
        out_specs=(P(None, "feat", None), P(), P(), P()),
        check_vma=False,
    )
```
